128 devices in a mesh: wide: 64 (over y, x, z), narrow: 2 (over core).
Axes of the slice: x: 4, y: 4, z: 4, core: 2. Of those that a mesh axis runs over, the one named last changes fastest.
Arguments:
- pool_tokens: bfloat16 [49152, 2048], P(('wide', 'narrow')), may hold values from -6 to 6
- cotangent: bfloat16 [98304, 2048], P(('wide', 'narrow')), may hold values from -6 to 6
- slot_weights: bfloat16 [128, 3, 2048, 512], P(('wide', 'narrow')), may hold values from -6 to 6
- row_index: int32 [128, 768], P(('wide', 'narrow')), may hold values from 0 to 383
- route_weight: float32 [128, 768], P(('wide', 'narrow')), may hold values from 0.05 to 1
- slot_expert: int32 [128, 1], replicated, may hold values from 0 to 7
- next_expert: int32 [128, 1], replicated, may hold values from 0 to 7
- master: float32 [8, 3, 2048, 512], P(None, None, ('wide', 'narrow')), may hold values from -6 to 6
- moment_m: float32 [8, 3, 2048, 512], P(None, None, ('wide', 'narrow')), may hold values from -4 to 4
- moment_v: float32 [8, 3, 2048, 512], P(None, None, ('wide', 'narrow')), may hold values from 0.05 to 1
Outputs:
- token_grads: bfloat16 [49152, 2048], P(('wide', 'narrow'))
- master_next: float32 [8, 3, 2048, 512], P(None, None, ('wide', 'narrow'))
- moment_m_next: float32 [8, 3, 2048, 512], P(None, None, ('wide', 'narrow'))
- moment_v_next: float32 [8, 3, 2048, 512], P(None, None, ('wide', 'narrow'))
- next_weights: bfloat16 [128, 3, 2048, 512], P(('wide', 'narrow'))
The draws below stay inside these ranges and needn't reach their ends.
Inputs may be any that keep to these rules, and one draw needn't show every extreme that they name: `slot_expert`: every one of the 8 experts is held by at least one slot; counts are uneven. `next_expert`: every one of the 8 experts is held by at least one slot; counts are uneven. `row_index`: indices into the pool of the slot's own device; a token may appear more than once.
All inputs are finite; a program needn't handle non-finite values.
Results may differ from the reference program's by a relative error of at most 0.0065.
Values may be sent and summed in bfloat16 or wider, within the bound.
No kernel may reach another device: no remote copies, remote signals or barrier semaphores. Data moves between devices by JAX's collectives and lax.ppermute only.
A program may use at most 128 MiB of HBM per device.

```python
import math
import jax
import jax.numpy as jnp
from jax import lax

D = 2048
H = 512
EXPERTS = 8
ROWS = 768
POOL = 384
SLOTS = 128
TOKENS = 49152
PACKED = 98304


def place_ends(result, stream_key, least, largest):
    spot = [jax.random.randint(jax.random.fold_in(stream_key, axis), (), 0, length) for axis, length in enumerate(result.shape)]
    longest = result.shape.index(max(result.shape))
    neighbour = spot[:longest] + [(spot[longest] + 1) % result.shape[longest]] + spot[longest + 1:]
    return result.at[tuple(spot)].set(least).at[tuple(neighbour)].set(largest)


def level_of(stream_key, shape, split, least, top_value):
    gain, own = 1.0, jax.random.fold_in(stream_key, 6)
    for position, shards_of in split:
        steps = jnp.exp(jax.random.uniform(jax.random.fold_in(own, position), (shards_of,), jnp.float32, least / len(split), top_value / len(split)))
        gain = gain * jnp.repeat(steps, shape[position] // shards_of).reshape([-1 if axis == position else 1 for axis in range(len(shape))])
    return gain


def different_ones(key, rows, number_of, top, lift):
    sequence = jax.random.permutation(jax.random.fold_in(key, 1), number_of)
    favour = sequence
    for power in range(3):
        favour = favour * favour // number_of
    favour = favour * lift // number_of
    chance = jax.random.randint(jax.random.fold_in(key, 2), (rows, number_of), 0, 4096) + favour
    sure = jax.random.permutation(jax.random.fold_in(key, 3), rows)[jnp.arange(number_of) % rows]
    chance = jnp.where(jnp.arange(rows)[:, None] == sure[None, :], 1 << 14, chance)
    score = chance * number_of + jnp.arange(number_of)
    return lax.top_k(score.astype(jnp.int32), top)[1].astype(jnp.int32)


def normal_values(own_key, shape, spread, bound, pieces=(), kind=jnp.bfloat16):
    drawn = spread * jax.random.normal(own_key, shape, jnp.float32)
    if pieces:
        drawn = drawn * level_of(own_key, shape, pieces, -0.22, 0.18)
    return jnp.clip(drawn, -bound, bound).astype(kind)


def setup_inputs(seed: int = 0) -> dict:
    key_list = jax.random.split(jax.random.key(seed), 11)
    return {
        "pool_tokens": normal_values(key_list[0], (TOKENS, D), 1.0, 6.0, ((0, 128),)),
        "cotangent": normal_values(key_list[1], (PACKED, D), 1.0, 6.0, ((0, 128),)),
        "slot_weights": normal_values(key_list[2], (SLOTS, 3, D, H), 1.0, 6.0, ((0, 128),)),
        "row_index": place_ends(jax.random.randint(key_list[3], (SLOTS, ROWS), 0, POOL), jax.random.fold_in(key_list[3], 1), 0, POOL - 1).astype(jnp.int32),
        "route_weight": jnp.clip(0.05 + 0.95 * jax.random.uniform(key_list[4], (SLOTS, ROWS), jnp.float32) ** level_of(key_list[4], (SLOTS, ROWS), ((0, 128),), -0.2, 0.2), 0.05, 1.0),
        "slot_expert": different_ones(key_list[5], SLOTS, EXPERTS, 1, 2048),
        "next_expert": different_ones(key_list[6], SLOTS, EXPERTS, 1, 2048),
        "master": normal_values(key_list[7], (EXPERTS, 3, D, H), 1.0, 6.0, ((2, 128),), jnp.float32),
        "moment_m": normal_values(key_list[8], (EXPERTS, 3, D, H), 0.3, 4.0, ((2, 128),), jnp.float32),
        "moment_v": jnp.clip(jnp.exp(math.log(1.0) - 2.9957323 * jax.random.uniform(key_list[9], (EXPERTS, 3, D, H), jnp.float32) ** level_of(key_list[9], (EXPERTS, 3, D, H), ((2, 128),), -0.2, 0.2)), 0.05, 1.0),
    }


def inner(left, right):
    return lax.dot_general(left, right, (((0,), (0,)), ((), ())), preferred_element_type=jnp.float32)

def against(left, right):
    return lax.dot_general(left, right, (((1,), (1,)), ((), ())), preferred_element_type=jnp.float32)

def slot_pass(rows, cotangent, weights, route):
    scale_in = weights.shape[1] ** (-0.5)
    scale_out = weights.shape[2] ** (-0.5)
    gate = jnp.dot(rows, weights[0], preferred_element_type=jnp.float32) * scale_in
    upper = jnp.dot(rows, weights[1], preferred_element_type=jnp.float32) * scale_in
    sigma = jax.nn.sigmoid(gate)
    active = gate * sigma
    hidden = (active * upper).astype(jnp.bfloat16)
    scaled = (route[:, None] * cotangent.astype(jnp.float32)).astype(jnp.bfloat16)
    back = jnp.dot(scaled, weights[2], preferred_element_type=jnp.float32) * scale_out
    d_gate = (back * upper * sigma * (1.0 + gate * (1.0 - sigma))).astype(jnp.bfloat16)
    d_up = (back * active).astype(jnp.bfloat16)
    grads = jnp.stack([inner(rows, d_gate) * scale_in, inner(rows, d_up) * scale_in, inner(scaled, hidden) * scale_out])
    inputs = (against(d_gate, weights[0]) + against(d_up, weights[1])) * scale_in
    return (grads, inputs)

def adam_step(grad, master, moment_m, moment_v):
    first = 0.9 * moment_m + 0.1 * grad
    second = 0.95 * moment_v + 0.05 * grad * grad
    fresh = master - 0.05 * (first / (jnp.sqrt(second) + 1e-08) + 0.1 * master)
    return (fresh, first, second)

def reference(pool_tokens, cotangent, slot_weights, row_index, route_weight, slot_expert, next_expert, master, moment_m, moment_v):
    pools = pool_tokens.reshape(SLOTS, POOL, D)
    cots = cotangent.reshape(SLOTS, ROWS, D)

    def visit(total, item):
        pool, cot, weights, index, route, expert = item
        rows = jnp.take(pool, index, axis=0)
        grads, inputs = slot_pass(rows, cot, weights, route)
        total = total.at[expert].add(grads)
        grad_pool = jnp.zeros((POOL, D), jnp.float32).at[index].add(inputs).astype(jnp.bfloat16)
        return (total, grad_pool)
    start = jnp.zeros((EXPERTS, 3, D, H), jnp.float32)
    total, grad_pools = lax.scan(visit, start, (pools, cots, slot_weights, row_index, route_weight, slot_expert[:, 0]))
    fresh, first, second = adam_step(total, master, moment_m, moment_v)
    next_weights = jnp.take(fresh.astype(jnp.bfloat16), next_expert[:, 0], axis=0)
    return (grad_pools.reshape(TOKENS, D), fresh, first, second, next_weights)
```

```python
import functools

import jax
import jax.numpy as jnp
from jax import lax
from jax.experimental import pallas as pl
from jax.experimental.pallas import tpu as pltpu
from jax.sharding import PartitionSpec as P

EXPERTS = 8
RING = 4
CORES = 2
STRIDES = (16, 4, 1)
BLOCK = 16
HIDDEN = 512
ORDERS = ((0, 1, 2), (1, 2, 0), (2, 0, 1))
BF16 = jnp.bfloat16
F32 = jnp.float32


VMEM = pl.BlockSpec(memory_space=pltpu.VMEM)
SMEM = pl.BlockSpec(memory_space=pltpu.SMEM)
ANY = pl.BlockSpec(memory_space=pl.ANY)


def moved(chip, axis, steps):
    stride = STRIDES[axis]
    here = (chip // stride) % RING
    return chip + ((here + steps) % RING - here) * stride


def shift(array, axis, steps, swap=0):
    chips = RING**3
    if swap:
        pairs = [
            (CORES * chip + core, CORES * moved(chip, axis, steps) + (core ^ 1))
            for chip in range(chips)
            for core in range(CORES)
        ]
        return lax.ppermute(array, ("wide", "narrow"), pairs)
    return lax.ppermute(array, "wide", [(chip, moved(chip, axis, steps)) for chip in range(chips)])


def at_axis(ranks, axis, index, *more):
    where = [slice(None)] * ranks
    where[axis] = index
    return tuple(where) + more


def rest(order):
    return sorted(order[1:])


def slot_of(pos, order, back_a, back_b, swap):
    spot = [pos[0], pos[1], pos[2]]
    spot[order[0]] = (spot[order[0]] - back_a) & (RING - 1)
    spot[order[1]] = (spot[order[1]] - back_b) & (RING - 1)
    chip = sum(s * stride for s, stride in zip(spot, STRIDES))
    return chip * CORES + (pos[3] ^ swap)


def cut_first(order, pos, grad, *outs):
    a = order[0]
    for steps in range(RING):
        for swap in range(CORES):
            target = (pos[a] + steps) & (RING - 1)
            outs[CORES * steps + swap][...] = grad[at_axis(3, a, target, pos[3] ^ swap)]


def cut_second(order, pos, *refs):
    ins, outs = refs[:8], refs[8:]
    b = order[1]
    dim = rest(order).index(b)
    for steps in range(RING):
        target = (pos[b] + steps) & (RING - 1)
        for k, piece in enumerate(ins):
            outs[steps][k] = piece[at_axis(2, dim, target)]


def sum_slots(order, pos, expert_of, *refs):
    ins, outs, total = refs[:4], refs[4:8], refs[8]
    d = order[2]
    total[...] = jnp.zeros_like(total)
    for back_b in range(RING):
        for k in range(RING * CORES):
            expert = expert_of[slot_of(pos, order, k // CORES, back_b, k % CORES)]
            for block in range(RING):
                total[block, expert] += ins[back_b][k, block].astype(F32)
    for steps in range(RING):
        target = (pos[d] + steps) & (RING - 1)
        outs[steps][...] = total[target].astype(outs[steps].dtype)


def adam(own, one, two, three, master, moment_m, moment_v, fresh, first, second, weights):
    grad = own[...] + one[...].astype(F32) + two[...].astype(F32) + three[...].astype(F32)
    m_next = 0.9 * moment_m[...] + 0.1 * grad
    v_next = 0.95 * moment_v[...] + 0.05 * grad * grad
    old = master[...]
    new = old - 0.05 * (m_next / (jnp.sqrt(v_next) + 1e-08) + 0.1 * old)
    fresh[...] = new
    first[...] = m_next
    second[...] = v_next
    weights[...] = new.astype(BF16)


def pick(order, pos, expert_of, *refs):
    ins, outs = refs[:4], refs[4:]
    b, d = order[1], order[2]
    b_first = rest(order)[0] == b
    for steps in range(RING):
        for swap in range(CORES):
            expert = expert_of[slot_of(pos, order, -steps, 0, swap)]
            for back_b in range(RING):
                for back_d in range(RING):
                    at_b = (pos[b] - back_b) & (RING - 1)
                    at_d = (pos[d] - back_d) & (RING - 1)
                    spot = (at_b, at_d) if b_first else (at_d, at_b)
                    outs[CORES * steps + swap][spot] = ins[back_b][back_d, expert]


def lay_out(order, part, pos, *refs):
    ins, out, sems = refs[:8], refs[-2], refs[-1]
    a = order[0]
    copies = []
    for k in range(RING * CORES):
        source = (pos[a] - k // CORES) & (RING - 1)
        spot = (part,) + at_axis(3, a, source, pos[3] ^ (k % CORES))
        copies.append(pltpu.make_async_copy(ins[k], out.at[spot], sems.at[k]))
    for copy in copies:
        copy.start()
    for copy in copies:
        copy.wait()


def shaped(shape, dtype=BF16):
    return jax.ShapeDtypeStruct(shape, dtype)


def call(body, outs, in_specs, args, **more):
    specs = more.pop("out_specs", [VMEM] * len(outs))
    return pl.pallas_call(body, out_shape=outs, in_specs=in_specs, out_specs=specs, **more)(*args)


def send_grads(grad, order, pos, slot_expert):
    a, b, d = order
    side = (RING, RING, BLOCK, HIDDEN)
    row = (RING * CORES, RING, BLOCK, HIDDEN)
    tile = (EXPERTS, BLOCK, HIDDEN)
    cut = grad.reshape(RING, RING, RING, CORES, BLOCK, HIDDEN)
    parts = call(
        functools.partial(cut_first, order), [shaped(side)] * 8, [SMEM, VMEM], (pos, cut)
    )
    got = [parts[k] if k == 0 else shift(parts[k], a, k // CORES, k % CORES) for k in range(8)]
    parts = call(
        functools.partial(cut_second, order), [shaped(row)] * 4, [SMEM] + [VMEM] * 8, (pos, *got)
    )
    got = [parts[0]] + [shift(parts[k], b, k) for k in range(1, RING)]
    parts = call(
        functools.partial(sum_slots, order),
        [shaped(tile, F32)] + [shaped(tile)] * 3,
        [SMEM, SMEM] + [VMEM] * 4,
        (pos, slot_expert, *got),
        scratch_shapes=[pltpu.VMEM((RING, *tile), F32)],
    )
    return [parts[0]] + [shift(parts[k], d, k) for k in range(1, RING)]


def update(grads, part, master, moment_m, moment_v):
    tile = (EXPERTS, BLOCK, HIDDEN)
    whole = pl.BlockSpec(tile, lambda i: (0, 0, 0))
    third = pl.BlockSpec((EXPERTS, None, BLOCK, HIDDEN), lambda i: (0, part, 0, 0))
    return call(
        adam,
        [shaped(tile, F32)] * 3 + [shaped(tile)],
        [whole] * 4 + [third] * 3,
        (*grads, master, moment_m, moment_v),
        out_specs=[whole] * 4,
        grid=(1,),
    )


def send_weights(weights, order, pos, next_expert):
    a, b, d = order
    side = (RING, RING, BLOCK, HIDDEN)
    line = jnp.stack([weights] + [shift(weights, d, k) for k in range(1, RING)])
    plane = [line] + [shift(line, b, k) for k in range(1, RING)]
    parts = call(
        functools.partial(pick, order),
        [shaped(side)] * 8,
        [SMEM, SMEM] + [VMEM] * 4,
        (pos, next_expert, *plane),
    )
    return [parts[k] if k == 0 else shift(parts[k], a, k // CORES, k % CORES) for k in range(8)]


def assemble(pieces, order, part, pos, into):
    whole = shaped((3, RING, RING, RING, CORES, BLOCK, HIDDEN))
    specs = [SMEM] + [ANY] * 8
    args = (pos, *pieces)
    alias = {}
    if into is not None:
        specs, args, alias = specs + [ANY], args + (into,), {9: 0}
    return call(
        functools.partial(lay_out, order, part),
        [whole],
        specs,
        args,
        out_specs=[ANY],
        scratch_shapes=[pltpu.SemaphoreType.DMA((8,))],
        input_output_aliases=alias,
    )[0]


def dot(left, right, dims):
    return lax.dot_general(left, right, ((dims[:1], dims[1:]), ((), ())), preferred_element_type=F32)


def local(
    pool_tokens,
    cotangent,
    slot_weights,
    row_index,
    route_weight,
    slot_expert,
    next_expert,
    master,
    moment_m,
    moment_v,
):
    chip = lax.axis_index("wide")
    pos = jnp.stack(
        [(chip // s) % RING for s in STRIDES] + [lax.axis_index("narrow")]
    ).astype(jnp.int32)
    slot_expert, next_expert = slot_expert[:, 0], next_expert[:, 0]
    wg, wu, wd = slot_weights[0, 0], slot_weights[0, 1], slot_weights[0, 2]
    scale_in = wg.shape[0] ** (-0.5)
    scale_out = wg.shape[1] ** (-0.5)
    pool = pool_tokens.shape[0]
    chosen = (row_index[0][:, None] == jnp.arange(pool, dtype=jnp.int32)[None, :]).astype(BF16)

    def spread(values):
        high = lax.reduce_precision(values, 8, 7)
        low = values - high
        return dot(chosen, high.astype(BF16), (1, 0)) + dot(chosen, low.astype(BF16), (1, 0))

    gate = spread(dot(pool_tokens, wg, (1, 0)) * scale_in)
    upper = spread(dot(pool_tokens, wu, (1, 0)) * scale_in)
    sigma = jax.nn.sigmoid(gate)
    active = gate * sigma
    hidden = (active * upper).astype(BF16)
    scaled = (route_weight[0][:, None] * cotangent.astype(F32)).astype(BF16)
    down_grad = (dot(scaled, hidden, (0, 0)) * scale_out).astype(BF16)
    back = dot(scaled, wd, (1, 0)) * scale_out
    d_gate = (back * upper * sigma * (1.0 + gate * (1.0 - sigma))).astype(BF16)
    d_up = (back * active).astype(BF16)
    gate_sum = dot(chosen, d_gate, (0, 0)).astype(BF16)
    up_sum = dot(chosen, d_up, (0, 0)).astype(BF16)
    gate_grad = (dot(pool_tokens, gate_sum, (0, 0)) * scale_in).astype(BF16)
    up_grad = (dot(pool_tokens, up_sum, (0, 0)) * scale_in).astype(BF16)
    token_grads = ((dot(gate_sum, wg, (1, 1)) + dot(up_sum, wu, (1, 1))) * scale_in).astype(BF16)

    results = {}
    out = None
    for part, grad in ((2, down_grad), (0, gate_grad), (1, up_grad)):
        with jax.named_scope(f"grads_{part}"):
            grads = send_grads(grad, ORDERS[part], pos, slot_expert)
        with jax.named_scope(f"adam_{part}"):
            results[part] = update(grads, part, master, moment_m, moment_v)
        with jax.named_scope(f"weights_{part}"):
            pieces = send_weights(results[part][3], ORDERS[part], pos, next_expert)
            out = assemble(pieces, ORDERS[part], part, pos, out)
    fresh, first, second = (
        jnp.stack([results[part][k] for part in range(3)], axis=1) for k in range(3)
    )
    next_weights = out.reshape(slot_weights.shape)
    return (token_grads, fresh, first, second, next_weights)


def solution(mesh):
    rows = P(("wide", "narrow"), None)
    cube = P(None, None, ("wide", "narrow"), None)
    slots = P(("wide", "narrow"), None, None, None)
    in_specs = (rows, rows, slots, rows, rows, P(), P(), cube, cube, cube)
    out_specs = (rows, cube, cube, cube, slots)
    return jax.shard_map(local, mesh=mesh, in_specs=in_specs, out_specs=out_specs, check_vma=False)
```

```python
import functools

import jax
import jax.numpy as jnp
from jax import lax
from jax.experimental import pallas as pl
from jax.experimental.pallas import tpu as pltpu
from jax.sharding import PartitionSpec as P

EXPERTS = 8
RING = 4
CORES = 2
STRIDES = (16, 4, 1)
BLOCK = 16
HIDDEN = 512
VMEM_BYTES = 9 * 2**20
ORDERS = ((0, 1, 2), (1, 2, 0), (2, 0, 1))
BF16 = jnp.bfloat16
F32 = jnp.float32


VMEM = pl.BlockSpec(memory_space=pltpu.VMEM)
SMEM = pl.BlockSpec(memory_space=pltpu.SMEM)
ANY = pl.BlockSpec(memory_space=pl.ANY)


def moved(chip, axis, steps):
    stride = STRIDES[axis]
    here = (chip // stride) % RING
    return chip + ((here + steps) % RING - here) * stride


def shift(array, axis, steps, swap=0):
    chips = RING**3
    if swap:
        pairs = [
            (CORES * chip + core, CORES * moved(chip, axis, steps) + (core ^ 1))
            for chip in range(chips)
            for core in range(CORES)
        ]
        return lax.ppermute(array, ("wide", "narrow"), pairs)
    return lax.ppermute(array, "wide", [(chip, moved(chip, axis, steps)) for chip in range(chips)])


def at_axis(ranks, axis, index, *more):
    where = [slice(None)] * ranks
    where[axis] = index
    return tuple(where) + more


def rest(order):
    return sorted(order[1:])


def slot_of(pos, order, back_a, back_b, swap):
    spot = [pos[0], pos[1], pos[2]]
    spot[order[0]] = (spot[order[0]] - back_a) & (RING - 1)
    spot[order[1]] = (spot[order[1]] - back_b) & (RING - 1)
    chip = sum(s * stride for s, stride in zip(spot, STRIDES))
    return chip * CORES + (pos[3] ^ swap)


def cut_first(order, pos, own, other, *outs):
    a = order[0]
    for steps in range(RING):
        target = (pos[a] + steps) & (RING - 1)
        for k, half in enumerate((own, other)):
            outs[steps][k] = half[at_axis(3, a, target)]


def cut_second(order, pos, *refs):
    ins, outs = refs[:RING], refs[RING:]
    b = order[1]
    dim = rest(order).index(b)
    for steps in range(RING):
        target = (pos[b] + steps) & (RING - 1)
        for back_a, piece in enumerate(ins):
            for k in range(CORES):
                outs[steps][CORES * back_a + k] = piece[(k,) + at_axis(2, dim, target)]


def sum_slots(order, pos, expert_of, *refs):
    ins, outs, total = refs[:4], refs[4:8], refs[8]
    d = order[2]
    total[...] = jnp.zeros_like(total)
    for back_b in range(RING):
        for k in range(RING * CORES):
            expert = expert_of[slot_of(pos, order, k // CORES, back_b, k % CORES)]
            for block in range(RING):
                total[block, expert] += ins[back_b][k, block].astype(F32)
    for steps in range(RING):
        target = (pos[d] + steps) & (RING - 1)
        outs[steps][...] = total[target].astype(outs[steps].dtype)


def adam(own, one, two, three, master, moment_m, moment_v, fresh, first, second, weights):
    grad = own[...] + one[...].astype(F32) + two[...].astype(F32) + three[...].astype(F32)
    m_next = 0.9 * moment_m[...] + 0.1 * grad
    v_next = 0.95 * moment_v[...] + 0.05 * grad * grad
    old = master[...]
    new = old - 0.05 * (m_next / (jnp.sqrt(v_next) + 1e-08) + 0.1 * old)
    fresh[...] = new
    first[...] = m_next
    second[...] = v_next
    weights[...] = new.astype(BF16)


def pick(order, pos, expert_of, *refs):
    ins, outs, sent = refs[:RING], refs[RING:-1], refs[-1]
    b, d = order[1], order[2]
    b_first = rest(order)[0] == b
    for steps in range(RING):
        for swap in range(CORES):
            expert = expert_of[slot_of(pos, order, -steps, 0, swap)]
            for back_b in range(RING):
                for back_d in range(RING):
                    at_b = (pos[b] - back_b) & (RING - 1)
                    at_d = (pos[d] - back_d) & (RING - 1)
                    spot = (at_b, at_d) if b_first else (at_d, at_b)
                    tile = ins[back_b][back_d, expert]
                    if swap:
                        sent[(steps,) + spot] = tile
                    else:
                        outs[steps][spot] = tile


def join(*refs):
    kept, other, outs = refs[:RING], refs[RING], refs[RING + 1 :]
    for steps in range(RING):
        outs[steps][0] = kept[steps][...]
        outs[steps][1] = other[steps]


def lay_out(order, pos, *refs):
    ins, out = refs[:RING], refs[-1]
    a = order[0]
    for back in range(RING):
        source = (pos[a] - back) & (RING - 1)
        for k in range(CORES):
            out[(0,) + at_axis(3, a, source, pos[3] ^ k)] = ins[back][k]


def shaped(shape, dtype=BF16):
    return jax.ShapeDtypeStruct(shape, dtype)


def call(body, outs, in_specs, args, **more):
    specs = more.pop("out_specs", [VMEM] * len(outs))
    return pl.pallas_call(
        body,
        out_shape=outs,
        in_specs=in_specs,
        out_specs=specs,
        compiler_params=pltpu.CompilerParams(vmem_limit_bytes=VMEM_BYTES),
        **more,
    )(*args)


def around(parts, axis):
    return [parts[0]] + [shift(parts[k], axis, k) for k in (1, 3, 2)]


def send_grads(grad, order, pos, slot_expert):
    a, b, d = order
    pair = (CORES, RING, RING, BLOCK, HIDDEN)
    row = (RING * CORES, RING, BLOCK, HIDDEN)
    tile = (EXPERTS, BLOCK, HIDDEN)
    cut = grad.reshape(RING, RING, RING, CORES, BLOCK, HIDDEN)
    own = lax.dynamic_index_in_dim(cut, pos[3], 3, keepdims=False)
    other = lax.dynamic_index_in_dim(cut, 1 - pos[3], 3, keepdims=False)
    other = lax.ppermute(other, "narrow", [(0, 1), (1, 0)])
    parts = call(
        functools.partial(cut_first, order),
        [shaped(pair)] * RING,
        [SMEM, VMEM, VMEM],
        (pos, own, other),
    )
    parts = around(parts, a)
    parts = call(
        functools.partial(cut_second, order),
        [shaped(row)] * RING,
        [SMEM] + [VMEM] * RING,
        (pos, parts[0], parts[1], parts[3], parts[2]),
    )
    parts = around(parts, b)
    parts = call(
        functools.partial(sum_slots, order),
        [shaped(tile, F32)] + [shaped(tile)] * 3,
        [SMEM, SMEM] + [VMEM] * RING,
        (pos, slot_expert, parts[0], parts[1], parts[3], parts[2]),
        scratch_shapes=[pltpu.VMEM((RING, *tile), F32)],
    )
    return around(parts, d)


def update(grads, part, master, moment_m, moment_v):
    tile = (EXPERTS, BLOCK, HIDDEN)
    whole = pl.BlockSpec(tile, lambda i: (0, 0, 0))
    third = pl.BlockSpec((EXPERTS, None, BLOCK, HIDDEN), lambda i: (0, part, 0, 0))
    return call(
        adam,
        [shaped(tile, F32)] * 3 + [shaped(tile)],
        [whole] * 4 + [third] * 3,
        (*grads, master, moment_m, moment_v),
        out_specs=[whole] * 4,
        grid=(1,),
    )


def send_weights(weights, order, pos, next_expert):
    a, b, d = order
    side = (RING, RING, BLOCK, HIDDEN)
    line = around([weights] * RING, d)
    line = jnp.stack([line[0], line[1], line[3], line[2]])
    plane = around([line] * RING, b)
    *kept, sent = call(
        functools.partial(pick, order),
        [shaped(side)] * RING + [shaped((RING, *side))],
        [SMEM, SMEM] + [VMEM] * RING,
        (pos, next_expert, plane[0], plane[1], plane[3], plane[2]),
    )
    other = lax.ppermute(sent, "narrow", [(0, 1), (1, 0)])
    parts = call(
        join, [shaped((CORES, *side))] * RING, [VMEM] * (RING + 1), (*kept, other)
    )
    parts = around(parts, a)
    return parts[0], parts[1], parts[3], parts[2]


def assemble(pieces, order, part, pos, into):
    dims = (3, RING, RING, RING, CORES, BLOCK, HIDDEN)
    specs = [SMEM] + [VMEM] * RING
    args = (pos, *pieces)
    alias = {}
    if into is not None:
        specs, args, alias = specs + [ANY], args + (into,), {RING + 1: 0}
    return call(
        functools.partial(lay_out, order),
        [shaped(dims)],
        specs,
        args,
        out_specs=[pl.BlockSpec((1, *dims[1:]), lambda i: (part,) + (0,) * 6)],
        grid=(1,),
        input_output_aliases=alias,
    )[0]


def dot(left, right, dims):
    return lax.dot_general(left, right, ((dims[:1], dims[1:]), ((), ())), preferred_element_type=F32)


def local(
    pool_tokens,
    cotangent,
    slot_weights,
    row_index,
    route_weight,
    slot_expert,
    next_expert,
    master,
    moment_m,
    moment_v,
):
    chip = lax.axis_index("wide")
    pos = jnp.stack(
        [(chip // s) % RING for s in STRIDES] + [lax.axis_index("narrow")]
    ).astype(jnp.int32)
    slot_expert, next_expert = slot_expert[:, 0], next_expert[:, 0]
    wg, wu, wd = slot_weights[0, 0], slot_weights[0, 1], slot_weights[0, 2]
    scale_in = wg.shape[0] ** (-0.5)
    scale_out = wg.shape[1] ** (-0.5)
    pool = pool_tokens.shape[0]
    chosen = (row_index[0][:, None] == jnp.arange(pool, dtype=jnp.int32)[None, :]).astype(BF16)

    def spread(values):
        high = lax.reduce_precision(values, 8, 7)
        low = values - high
        return dot(chosen, high.astype(BF16), (1, 0)) + dot(chosen, low.astype(BF16), (1, 0))

    gate = spread(dot(pool_tokens, wg, (1, 0)) * scale_in)
    upper = spread(dot(pool_tokens, wu, (1, 0)) * scale_in)
    sigma = jax.nn.sigmoid(gate)
    active = gate * sigma
    hidden = (active * upper).astype(BF16)
    scaled = (route_weight[0][:, None] * cotangent.astype(F32)).astype(BF16)
    down_grad = (dot(scaled, hidden, (0, 0)) * scale_out).astype(BF16)
    back = dot(scaled, wd, (1, 0)) * scale_out
    d_gate = (back * upper * sigma * (1.0 + gate * (1.0 - sigma))).astype(BF16)
    d_up = (back * active).astype(BF16)
    gate_sum = dot(chosen, d_gate, (0, 0)).astype(BF16)
    up_sum = dot(chosen, d_up, (0, 0)).astype(BF16)
    gate_grad = (dot(pool_tokens, gate_sum, (0, 0)) * scale_in).astype(BF16)
    up_grad = (dot(pool_tokens, up_sum, (0, 0)) * scale_in).astype(BF16)
    token_grads = ((dot(gate_sum, wg, (1, 1)) + dot(up_sum, wu, (1, 1))) * scale_in).astype(BF16)

    results = {}
    out = None
    for part, grad in ((2, down_grad), (0, gate_grad), (1, up_grad)):
        with jax.named_scope(f"grads_{part}"):
            grads = send_grads(grad, ORDERS[part], pos, slot_expert)
        with jax.named_scope(f"adam_{part}"):
            results[part] = update(grads, part, master, moment_m, moment_v)
        with jax.named_scope(f"weights_{part}"):
            pieces = send_weights(results[part][3], ORDERS[part], pos, next_expert)
            out = assemble(pieces, ORDERS[part], part, pos, out)
    fresh, first, second = (
        jnp.stack([results[part][k] for part in range(3)], axis=1) for k in range(3)
    )
    next_weights = out.reshape(slot_weights.shape)
    return (token_grads, fresh, first, second, next_weights)


def solution(mesh):
    rows = P(("wide", "narrow"), None)
    cube = P(None, None, ("wide", "narrow"), None)
    slots = P(("wide", "narrow"), None, None, None)
    in_specs = (rows, rows, slots, rows, rows, P(), P(), cube, cube, cube)
    out_specs = (rows, cube, cube, cube, slots)
    return jax.shard_map(local, mesh=mesh, in_specs=in_specs, out_specs=out_specs, check_vma=False)
```

```python
import functools

import jax
import jax.numpy as jnp
from jax import lax
from jax.experimental import pallas as pl
from jax.experimental.pallas import tpu as pltpu
from jax.sharding import PartitionSpec as P

EXPERTS = 8
RING = 4
CORES = 2
STRIDES = (16, 4, 1)
BLOCK = 16
HIDDEN = 512
VMEM_BYTES = 9 * 2**20
ORDERS = ((0, 1, 2), (1, 2, 0), (2, 0, 1))
BF16 = jnp.bfloat16
F32 = jnp.float32


VMEM = pl.BlockSpec(memory_space=pltpu.VMEM)
SMEM = pl.BlockSpec(memory_space=pltpu.SMEM)
ANY = pl.BlockSpec(memory_space=pl.ANY)
HBM = pl.BlockSpec(memory_space=pltpu.HBM)


def moved(chip, axis, steps):
    stride = STRIDES[axis]
    here = (chip // stride) % RING
    return chip + ((here + steps) % RING - here) * stride


def shift(array, axis, steps, swap=0):
    chips = RING**3
    if swap:
        pairs = [
            (CORES * chip + core, CORES * moved(chip, axis, steps) + (core ^ 1))
            for chip in range(chips)
            for core in range(CORES)
        ]
        return lax.ppermute(array, ("wide", "narrow"), pairs)
    return lax.ppermute(array, "wide", [(chip, moved(chip, axis, steps)) for chip in range(chips)])


def at_axis(ranks, axis, index, *more):
    where = [slice(None)] * ranks
    where[axis] = index
    return tuple(where) + more


def rest(order):
    return sorted(order[1:])


def slot_of(pos, order, back_a, back_b, swap):
    spot = [pos[0], pos[1], pos[2]]
    spot[order[0]] = (spot[order[0]] - back_a) & (RING - 1)
    spot[order[1]] = (spot[order[1]] - back_b) & (RING - 1)
    chip = sum(s * stride for s, stride in zip(spot, STRIDES))
    return chip * CORES + (pos[3] ^ swap)


def cut_first(order, pos, own, other, *outs):
    a = order[0]
    for steps in range(RING):
        target = (pos[a] + steps) & (RING - 1)
        for k, half in enumerate((own, other)):
            outs[steps][k] = half[at_axis(3, a, target)]


def cut_second(order, pos, *refs):
    ins, outs = refs[:RING], refs[RING:]
    b = order[1]
    dim = rest(order).index(b)
    for steps in range(RING):
        target = (pos[b] + steps) & (RING - 1)
        for back_a, piece in enumerate(ins):
            for k in range(CORES):
                outs[steps][CORES * back_a + k] = piece[(k,) + at_axis(2, dim, target)]


def sum_slots(order, pos, expert_of, *refs):
    ins, outs, total = refs[:4], refs[4:8], refs[8]
    d = order[2]
    total[...] = jnp.zeros_like(total)
    for back_b in range(RING):
        for k in range(RING * CORES):
            expert = expert_of[slot_of(pos, order, k // CORES, back_b, k % CORES)]
            for block in range(RING):
                total[block, expert] += ins[back_b][k, block].astype(F32)
    for steps in range(RING):
        target = (pos[d] + steps) & (RING - 1)
        outs[steps][...] = total[target].astype(outs[steps].dtype)


def adam(own, one, two, three, master, moment_m, moment_v, fresh, first, second, weights):
    grad = own[...] + one[...].astype(F32) + two[...].astype(F32) + three[...].astype(F32)
    m_next = 0.9 * moment_m[...] + 0.1 * grad
    v_next = 0.95 * moment_v[...] + 0.05 * grad * grad
    old = master[...]
    new = old - 0.05 * (m_next / (jnp.sqrt(v_next) + 1e-08) + 0.1 * old)
    fresh[...] = new
    first[...] = m_next
    second[...] = v_next
    weights[...] = new.astype(BF16)


def pick(order, pos, expert_of, *refs):
    ins, outs, sent = refs[:RING], refs[RING:-1], refs[-1]
    b, d = order[1], order[2]
    b_first = rest(order)[0] == b
    for steps in range(RING):
        for swap in range(CORES):
            expert = expert_of[slot_of(pos, order, -steps, 0, swap)]
            for back_b in range(RING):
                for back_d in range(RING):
                    at_b = (pos[b] - back_b) & (RING - 1)
                    at_d = (pos[d] - back_d) & (RING - 1)
                    spot = (at_b, at_d) if b_first else (at_d, at_b)
                    tile = ins[back_b][back_d, expert]
                    if swap:
                        sent[(steps,) + spot] = tile
                    else:
                        outs[steps][spot] = tile


def join(*refs):
    kept, other, outs = refs[:RING], refs[RING], refs[RING + 1 :]
    for steps in range(RING):
        outs[steps][0] = kept[steps][...]
        outs[steps][1] = other[steps]


def lay_out(order, pos, *refs):
    ins, out = refs[:RING], refs[-1]
    a = order[0]
    for back in range(RING):
        source = (pos[a] - back) & (RING - 1)
        for k in range(CORES):
            out[(0,) + at_axis(3, a, source, pos[3] ^ k)] = ins[back][k]


def shaped(shape, dtype=BF16):
    return jax.ShapeDtypeStruct(shape, dtype)


def call(body, outs, in_specs, args, limit=VMEM_BYTES, work=0, **more):
    specs = more.pop("out_specs", [VMEM] * len(outs))
    return pl.pallas_call(
        body,
        out_shape=outs,
        in_specs=in_specs,
        out_specs=specs,
        compiler_params=pltpu.CompilerParams(vmem_limit_bytes=limit),
        cost_estimate=pl.CostEstimate(flops=work, bytes_accessed=0, transcendentals=0),
        **more,
    )(*args)


def around(parts, axis):
    got = [parts[0]]
    for k in (1, 3, 2):
        got.append(shift(parts[k], axis, k))
    return got


def start_grads(own, other, order, pos):
    pair = (CORES, RING, RING, BLOCK, HIDDEN)
    cube = (RING, RING, RING, BLOCK, HIDDEN)
    other = lax.ppermute(other, "narrow", [(0, 1), (1, 0)])
    return call(
        functools.partial(cut_first, order),
        [shaped(pair)] * RING,
        [SMEM, VMEM, VMEM],
        (pos, own.reshape(cube), other.reshape(cube)),
    )


def send_grads(parts, order, pos, slot_expert):
    a, b, d = order
    row = (RING * CORES, RING, BLOCK, HIDDEN)
    tile = (EXPERTS, BLOCK, HIDDEN)
    parts = around(parts, a)
    parts = call(
        functools.partial(cut_second, order),
        [shaped(row)] * RING,
        [SMEM] + [VMEM] * RING,
        (pos, parts[0], parts[1], parts[3], parts[2]),
    )
    parts = around(parts, b)
    parts = call(
        functools.partial(sum_slots, order),
        [shaped(tile, F32)] + [shaped(tile)] * 3,
        [SMEM, SMEM] + [VMEM] * RING,
        (pos, slot_expert, parts[0], parts[1], parts[3], parts[2]),
        scratch_shapes=[pltpu.VMEM((RING, *tile), F32)],
    )
    return around(parts, d)


def update(grads, part, master, moment_m, moment_v):
    tile = (EXPERTS, BLOCK, HIDDEN)
    whole = pl.BlockSpec(tile, lambda i: (0, 0, 0))
    third = pl.BlockSpec((EXPERTS, None, BLOCK, HIDDEN), lambda i: (0, part, 0, 0))
    return call(
        adam,
        [shaped(tile, F32)] * 3 + [shaped(tile)],
        [whole] * 4 + [third] * 3,
        (*grads, master, moment_m, moment_v),
        out_specs=[whole] * 4,
        grid=(1,),
    )


def send_weights(weights, order, pos, next_expert):
    a, b, d = order
    side = (RING, RING, BLOCK, HIDDEN)
    line = around([weights] * RING, d)
    line = jnp.stack([line[0], line[1], line[3], line[2]])
    plane = around([line] * RING, b)
    *kept, sent = call(
        functools.partial(pick, order),
        [shaped(side)] * RING + [shaped((RING, *side))],
        [SMEM, SMEM] + [VMEM] * RING,
        (pos, next_expert, plane[0], plane[1], plane[3], plane[2]),
    )
    other = lax.ppermute(sent, "narrow", [(0, 1), (1, 0)])
    parts = call(
        join, [shaped((CORES, *side))] * RING, [VMEM] * (RING + 1), (*kept, other)
    )
    parts = around(parts, a)
    return parts[0], parts[1], parts[3], parts[2]


def assemble(pieces, order, part, pos, into):
    dims = (3, RING, RING, RING, CORES, BLOCK, HIDDEN)
    specs = [SMEM] + [VMEM] * RING
    args = (pos, *pieces)
    alias = {}
    if into is not None:
        specs, args, alias = specs + [ANY], args + (into,), {RING + 1: 0}
    return call(
        functools.partial(lay_out, order),
        [shaped(dims)],
        specs,
        args,
        out_specs=[pl.BlockSpec((1, *dims[1:]), lambda i: (part,) + (0,) * 6)],
        grid=(1,),
        input_output_aliases=alias,
    )[0]


def mul(left, right, dims):
    return lax.dot_general(left, right, ((dims[:1], dims[1:]), ((), ())), preferred_element_type=F32)


def rows_of(count, size):
    return [slice(k, k + size) for k in range(0, count, size)]


def forward(pos, index, route, pool_in, weights_in, cot_in, own, other, gate, upper, scaled,
            pool, wg, wu, cot, high, low, hidden, grad, sems):
    pairs = (
        (pool_in, pool),
        (weights_in.at[0, 0], wg),
        (weights_in.at[0, 1], wu),
        (cot_in, cot),
    )
    copies = [pltpu.make_async_copy(a, b, sems.at[k]) for k, (a, b) in enumerate(pairs)]
    for copy in copies:
        copy.start()
    width, hidden_units = wg.shape
    scale_in, scale_out = width ** (-0.5), hidden_units ** (-0.5)
    copies[0].wait()
    for k, w in enumerate((wg, wu)):
        copies[1 + k].wait()
        values = mul(pool[...], w[...], (1, 0)) * scale_in
        top = values.astype(BF16)
        high[k] = top
        low[k] = (values - top.astype(F32)).astype(BF16)
    for r in rows_of(index.shape[0], 256):
        spots = lax.broadcasted_iota(jnp.int32, (256, pool.shape[0]), 1)
        chosen = jnp.where(index[r, :] == spots, 1.0, 0.0).astype(BF16)
        for k, out in enumerate((gate, upper)):
            out[r, :] = mul(chosen, high[k], (1, 0)) + mul(chosen, low[k], (1, 0))

    def activate(step, carry):
        r = pl.ds(pl.multiple_of(step * 64, 64), 64)
        g = gate[r, :]
        hidden[r, :] = (g * jax.nn.sigmoid(g) * upper[r, :]).astype(BF16)
        return carry

    lax.fori_loop(0, index.shape[0] // 64, activate, 0)
    copies[3].wait()

    def scale(step, carry):
        r = pl.ds(pl.multiple_of(step * 32, 32), 32)
        scaled[r, :] = (route[r, :] * cot[r, :].astype(F32)).astype(BF16)
        return carry

    lax.fori_loop(0, index.shape[0] // 32, scale, 0)
    blocks = hidden_units // (BLOCK * CORES)
    for k, r in enumerate(rows_of(width, hidden_units)):
        values = mul(scaled[:, r], hidden[...], (0, 0)) * scale_out
        grad[k * blocks:(k + 1) * blocks] = values.astype(BF16).reshape(blocks, CORES, BLOCK, hidden_units)
    own[...] = grad[:, pos[3]]
    other[...] = grad[:, 1 - pos[3]]


def backward(index, gate, upper, scaled, weights_in, gate_sum, up_sum, wd, d_gate, d_up, sem):
    copy = pltpu.make_async_copy(weights_in.at[0, 2], wd, sem)
    copy.start()
    spots = lax.broadcasted_iota(jnp.int32, (gate_sum.shape[0], index.shape[1]), 0)
    chosen = jnp.where(index[...] == spots, 1.0, 0.0).astype(BF16)
    copy.wait()
    scale_out = wd.shape[1] ** (-0.5)
    for r in rows_of(gate.shape[0], 256):
        back = mul(scaled[r, :], wd[...], (1, 0)) * scale_out
        g = gate[r, :]
        sigma = jax.nn.sigmoid(g)
        d_gate[r, :] = (back * upper[r, :] * sigma * (1.0 + g * (1.0 - sigma))).astype(BF16)
        d_up[r, :] = (back * (g * sigma)).astype(BF16)
    gate_sum[...] = mul(chosen, d_gate[...], (1, 0)).astype(BF16)
    up_sum[...] = mul(chosen, d_up[...], (1, 0)).astype(BF16)


def pool_grads(pos, pool, gate_sum, up_sum, gate_own, gate_other, up_own, up_other, grad):
    width, hidden_units = pool.shape[1], gate_sum.shape[1]
    scale_in = width ** (-0.5)
    blocks = hidden_units // (BLOCK * CORES)
    for total, own, other in ((gate_sum, gate_own, gate_other), (up_sum, up_own, up_other)):
        for k, r in enumerate(rows_of(width, hidden_units)):
            values = (mul(pool[:, r], total[...], (0, 0)) * scale_in).astype(BF16)
            grad[k * blocks : (k + 1) * blocks] = values.reshape(
                blocks, CORES, BLOCK, hidden_units
            )
        own[...] = grad[:, pos[3]]
        other[...] = grad[:, 1 - pos[3]]


def run_forward(pos, index, route, pool, weights, cot):
    rows, width = cot.shape
    tokens, hid = pool.shape[0], weights.shape[3]
    half = (width // (BLOCK * CORES), BLOCK, hid)
    return call(
        forward,
        [shaped(half)] * 2 + [shaped((rows, hid), F32)] * 2 + [shaped((rows, width))],
        [SMEM, VMEM, VMEM, HBM, HBM, HBM],
        (pos, index.reshape(-1, 1), route.reshape(-1, 1), pool, weights, cot),
        scratch_shapes=[
            pltpu.VMEM(pool.shape, BF16),
            pltpu.VMEM((width, hid), BF16),
            pltpu.VMEM((width, hid), BF16),
            pltpu.VMEM(cot.shape, BF16),
            pltpu.VMEM((2, tokens, hid), BF16),
            pltpu.VMEM((2, tokens, hid), BF16),
            pltpu.VMEM((rows, hid), BF16),
            pltpu.VMEM((half[0], CORES, BLOCK, hid), BF16),
            pltpu.SemaphoreType.DMA((4,)),
        ],
        limit=47 * 2**20,
        work=5 * 10**9,
    )


def run_backward(index, gate, upper, scaled, weights, tokens):
    rows, width = scaled.shape
    hid = weights.shape[3]
    return call(
        backward,
        [shaped((tokens, hid))] * 2,
        [VMEM] * 4 + [HBM],
        (index, gate, upper, scaled, weights),
        scratch_shapes=[
            pltpu.VMEM((width, hid), BF16),
            pltpu.VMEM((rows, hid), BF16),
            pltpu.VMEM((rows, hid), BF16),
            pltpu.SemaphoreType.DMA,
        ],
        limit=50 * 2**20,
        work=3 * 10**9,
    )


def run_pool_grads(pos, pool, gate_sum, up_sum):
    width, hid = pool.shape[1], gate_sum.shape[1]
    half = (width // (BLOCK * CORES), BLOCK, hid)
    return call(
        pool_grads,
        [shaped(half)] * 4,
        [SMEM, VMEM, VMEM, VMEM],
        (pos, pool, gate_sum, up_sum),
        scratch_shapes=[pltpu.VMEM((half[0], CORES, BLOCK, hid), BF16)],
        limit=20 * 2**20,
        work=2 * 10**9,
    )


def local(
    pool_tokens,
    cotangent,
    slot_weights,
    row_index,
    route_weight,
    slot_expert,
    next_expert,
    master,
    moment_m,
    moment_v,
):
    chip = lax.axis_index("wide")
    pos = jnp.stack(
        [(chip // s) % RING for s in STRIDES] + [lax.axis_index("narrow")]
    ).astype(jnp.int32)
    slot_expert, next_expert = slot_expert[:, 0], next_expert[:, 0]
    weights_in = slot_weights
    scale_in = pool_tokens.shape[1] ** (-0.5)
    tokens = pool_tokens.shape[0]
    own, other, gate, upper, scaled = run_forward(
        pos, row_index, route_weight, pool_tokens, weights_in, cotangent
    )
    cut = {2: start_grads(own, other, ORDERS[2], pos)}
    gate_sum, up_sum = run_backward(row_index, gate, upper, scaled, weights_in, tokens)
    cut[2], (gate_sum, up_sum) = lax.optimization_barrier((cut[2], (gate_sum, up_sum)))
    own_0, other_0, own_1, other_1 = run_pool_grads(pos, pool_tokens, gate_sum, up_sum)
    cut[0] = start_grads(own_0, other_0, ORDERS[0], pos)
    cut[1] = start_grads(own_1, other_1, ORDERS[1], pos)
    token_grads = (
        mul(gate_sum, weights_in[0, 0], (1, 1)) + mul(up_sum, weights_in[0, 1], (1, 1))
    ) * scale_in
    token_grads = token_grads.astype(BF16)

    results = {}
    out = None
    for part in (2, 0, 1):
        grads = send_grads(cut[part], ORDERS[part], pos, slot_expert)
        results[part] = update(grads, part, master, moment_m, moment_v)
        pieces = send_weights(results[part][3], ORDERS[part], pos, next_expert)
        out = assemble(pieces, ORDERS[part], part, pos, out)
    fresh, first, second = (
        jnp.stack([results[part][k] for part in range(3)], axis=1) for k in range(3)
    )
    next_weights = out.reshape(slot_weights.shape)
    return (token_grads, fresh, first, second, next_weights)


def solution(mesh):
    rows = P(("wide", "narrow"), None)
    cube = P(None, None, ("wide", "narrow"), None)
    slots = P(("wide", "narrow"), None, None, None)
    in_specs = (rows, rows, slots, rows, rows, P(), P(), cube, cube, cube)
    out_specs = (rows, cube, cube, cube, slots)
    return jax.shard_map(local, mesh=mesh, in_specs=in_specs, out_specs=out_specs, check_vma=False)
```

```python
import functools

import jax
import jax.numpy as jnp
from jax import lax
from jax.experimental import pallas as pl
from jax.experimental.pallas import tpu as pltpu
from jax.sharding import PartitionSpec as P

EXPERTS = 8
RING = 4
CORES = 2
STRIDES = (16, 4, 1)
BLOCK = 16
HIDDEN = 512
LANES = 128
VMEM_BYTES = 9 * 2**20
ORDERS = ((0, 1, 2), (1, 2, 0), (2, 0, 1))
BF16 = jnp.bfloat16
F32 = jnp.float32


VMEM = pl.BlockSpec(memory_space=pltpu.VMEM)
SMEM = pl.BlockSpec(memory_space=pltpu.SMEM)
ANY = pl.BlockSpec(memory_space=pl.ANY)
HBM = pl.BlockSpec(memory_space=pltpu.HBM)


def moved(chip, axis, steps):
    stride = STRIDES[axis]
    here = (chip // stride) % RING
    return chip + ((here + steps) % RING - here) * stride


def shift(array, axis, steps, swap=0):
    chips = RING**3
    if swap:
        pairs = [
            (CORES * chip + core, CORES * moved(chip, axis, steps) + (core ^ 1))
            for chip in range(chips)
            for core in range(CORES)
        ]
        return lax.ppermute(array, ("wide", "narrow"), pairs)
    return lax.ppermute(array, "wide", [(chip, moved(chip, axis, steps)) for chip in range(chips)])


def at_axis(ranks, axis, index, *more):
    where = [slice(None)] * ranks
    where[axis] = index
    return tuple(where) + more


def rest(order):
    return sorted(order[1:])


def slot_of(pos, order, back_a, back_b, swap):
    spot = [pos[0], pos[1], pos[2]]
    spot[order[0]] = (spot[order[0]] - back_a) & (RING - 1)
    spot[order[1]] = (spot[order[1]] - back_b) & (RING - 1)
    chip = sum(s * stride for s, stride in zip(spot, STRIDES))
    return chip * CORES + (pos[3] ^ swap)


def cut_first(order, pos, own, other, *outs):
    a = order[0]

    def step(i, carry):
        for steps in range(RING):
            target = (pos[a] + steps) & (RING - 1)
            for k, half in enumerate((own, other)):
                where = (target, i) if a == 0 else (i, *at_axis(2, a - 1, target))
                outs[steps][k, i] = half[where]
        return carry

    lax.fori_loop(0, RING, step, 0)


def cut_second(order, pos, *refs):
    ins, outs = refs[:RING], refs[RING:]
    b = order[1]
    dim = rest(order).index(b)
    for steps in range(RING):
        target = (pos[b] + steps) & (RING - 1)
        for back_a, piece in enumerate(ins):
            for k in range(CORES):
                outs[steps][CORES * back_a + k] = piece[(k,) + at_axis(2, dim, target)]


def sum_slots(order, pos, expert_of, *refs):
    ins, outs, total = refs[:4], refs[4:8], refs[8]
    d = order[2]
    total[...] = jnp.zeros_like(total)
    for back_b in range(RING):
        for k in range(RING * CORES):
            expert = expert_of[slot_of(pos, order, k // CORES, back_b, k % CORES)]

            def add(block, carry, expert=expert, piece=ins[back_b].at[k]):
                total[block, expert] += piece[block].astype(F32)
                return carry

            lax.fori_loop(0, RING, add, 0)
    for steps in range(RING):
        target = (pos[d] + steps) & (RING - 1)
        outs[steps][...] = total[target].astype(outs[steps].dtype)


def adam(own, one, two, three, master, moment_m, moment_v, fresh, first, second, weights):
    grad = own[...] + one[...].astype(F32) + two[...].astype(F32) + three[...].astype(F32)
    m_next = 0.9 * moment_m[...] + 0.1 * grad
    v_next = 0.95 * moment_v[...] + 0.05 * grad * grad
    old = master[...]
    new = old - 0.05 * (m_next / (jnp.sqrt(v_next) + 1e-08) + 0.1 * old)
    fresh[...] = new
    first[...] = m_next
    second[...] = v_next
    weights[...] = new.astype(BF16)


def pick(order, pos, expert_of, *refs):
    ins, outs, sent = refs[:RING], refs[RING:-1], refs[-1]
    b, d = order[1], order[2]
    b_first = rest(order)[0] == b
    for steps in range(RING):
        for swap in range(CORES):
            expert = expert_of[slot_of(pos, order, -steps, 0, swap)]
            for back_b in range(RING):
                for back_d in range(RING):
                    at_b = (pos[b] - back_b) & (RING - 1)
                    at_d = (pos[d] - back_d) & (RING - 1)
                    spot = (at_b, at_d) if b_first else (at_d, at_b)
                    tile = ins[back_b][back_d, expert]
                    if swap:
                        sent[(steps,) + spot] = tile
                    else:
                        outs[steps][spot] = tile


def join(*refs):
    kept, other, outs = refs[:RING], refs[RING], refs[RING + 1 :]
    for steps in range(RING):
        outs[steps][0] = kept[steps][...]
        outs[steps][1] = other[steps]


def lay_out(order, pos, *refs):
    ins, out = refs[:RING], refs[-1]
    a = order[0]
    for back in range(RING):
        source = (pos[a] - back) & (RING - 1)
        for k in range(CORES):
            out[(0,) + at_axis(3, a, source, pos[3] ^ k)] = ins[back][k]


def shaped(shape, dtype=BF16):
    return jax.ShapeDtypeStruct(shape, dtype)


def call(body, outs, in_specs, args, limit=VMEM_BYTES, work=0, **more):
    specs = more.pop("out_specs", [VMEM] * len(outs))
    return pl.pallas_call(
        body,
        out_shape=outs,
        in_specs=in_specs,
        out_specs=specs,
        compiler_params=pltpu.CompilerParams(vmem_limit_bytes=limit),
        cost_estimate=pl.CostEstimate(flops=work, bytes_accessed=0, transcendentals=0),
        **more,
    )(*args)


def around(parts, axis):
    got = [parts[0]]
    for k in (2, 1, 3):
        got.append(shift(parts[k], axis, k))
    return got


def start_grads(own, other, order, pos):
    pair = (CORES, RING, RING, BLOCK, HIDDEN)
    cube = (RING, RING, RING, BLOCK, HIDDEN)
    other = lax.ppermute(other, "narrow", [(0, 1), (1, 0)])
    return call(
        functools.partial(cut_first, order),
        [shaped(pair)] * RING,
        [SMEM, VMEM, VMEM],
        (pos, own.reshape(cube), other.reshape(cube)),
    )


def send_grads(parts, order, pos, slot_expert):
    a, b, d = order
    row = (RING * CORES, RING, BLOCK, HIDDEN)
    tile = (EXPERTS, BLOCK, HIDDEN)
    parts = around(parts, a)
    parts = call(
        functools.partial(cut_second, order),
        [shaped(row)] * RING,
        [SMEM] + [VMEM] * RING,
        (pos, parts[0], parts[2], parts[1], parts[3]),
    )
    parts = around(parts, b)
    parts = call(
        functools.partial(sum_slots, order),
        [shaped(tile, F32)] + [shaped(tile)] * 3,
        [SMEM, SMEM] + [VMEM] * RING,
        (pos, slot_expert, parts[0], parts[2], parts[1], parts[3]),
        scratch_shapes=[pltpu.VMEM((RING, *tile), F32)],
    )
    return around(parts, d)


def update(grads, part, master, moment_m, moment_v):
    tile = (EXPERTS, BLOCK, HIDDEN)
    whole = pl.BlockSpec(tile, lambda i: (0, 0, 0))
    third = pl.BlockSpec((EXPERTS, None, BLOCK, HIDDEN), lambda i: (0, part, 0, 0))
    return call(
        adam,
        [shaped(tile, F32)] * 3 + [shaped(tile)],
        [whole] * 4 + [third] * 3,
        (*grads, master, moment_m, moment_v),
        out_specs=[whole] * 4,
        grid=(1,),
    )


def send_weights(weights, order, pos, next_expert):
    a, b, d = order
    side = (RING, RING, BLOCK, HIDDEN)
    line = around([weights] * RING, d)
    line = jnp.stack([line[0], line[2], line[1], line[3]])
    plane = around([line] * RING, b)
    *kept, sent = call(
        functools.partial(pick, order),
        [shaped(side)] * RING + [shaped((RING, *side))],
        [SMEM, SMEM] + [VMEM] * RING,
        (pos, next_expert, plane[0], plane[2], plane[1], plane[3]),
    )
    other = lax.ppermute(sent, "narrow", [(0, 1), (1, 0)])
    parts = call(
        join, [shaped((CORES, *side))] * RING, [VMEM] * (RING + 1), (*kept, other)
    )
    parts = around(parts, a)
    return parts[0], parts[2], parts[1], parts[3]


def assemble(pieces, order, part, pos, into):
    dims = (3, RING, RING, RING, CORES, BLOCK, HIDDEN)
    specs = [SMEM] + [VMEM] * RING
    args = (pos, *pieces)
    alias = {}
    if into is not None:
        specs, args, alias = specs + [ANY], args + (into,), {RING + 1: 0}
    return call(
        functools.partial(lay_out, order),
        [shaped(dims)],
        specs,
        args,
        out_specs=[pl.BlockSpec((1, *dims[1:]), lambda i: (part,) + (0,) * 6)],
        grid=(1,),
        input_output_aliases=alias,
    )[0]


def mul(left, right, dims):
    return lax.dot_general(left, right, ((dims[:1], dims[1:]), ((), ())), preferred_element_type=F32)


def down_columns(row):
    return jnp.transpose(jnp.broadcast_to(row, (LANES, row.shape[1])))


def forward(pos, index, route, pool, weights_in, cot_in, own, other, gate, upper, scaled, wd,
            wg, wu, cot, spot, factor, high, low, hidden, grad, sems):
    pairs = (
        (weights_in.at[0, 0], wg),
        (weights_in.at[0, 1], wu),
        (cot_in, cot),
        (weights_in.at[0, 2], wd),
    )
    copies = [pltpu.make_async_copy(a, b, sems.at[k]) for k, (a, b) in enumerate(pairs)]
    copies[0].start()
    width, hidden_units = wg.shape
    rows = index.shape[1]
    scale_in, scale_out = width ** (-0.5), hidden_units ** (-0.5)
    spot[...] = down_columns(index[...].astype(F32))
    factor[...] = down_columns(route[...])
    for k, w in enumerate((wg, wu)):
        copies[k].wait()
        copies[k + 1].start()
        values = mul(pool[...], w[...], (1, 0)) * scale_in
        top = values.astype(BF16)
        high[k] = top
        low[k] = (values - top.astype(F32)).astype(BF16)
    lanes = lax.broadcasted_iota(jnp.int32, (256, LANES), 1).astype(F32)

    def expand(step, carry):
        r = pl.ds(pl.multiple_of(step * 256, 256), 256)
        chosen = jnp.concatenate(
            [
                jnp.where(spot[r, :] == lanes + float(k), 1.0, 0.0).astype(BF16)
                for k in range(0, pool.shape[0], LANES)
            ],
            axis=1,
        )
        for k, out in enumerate((gate, upper)):
            out[r, :] = mul(chosen, high[k], (1, 0)) + mul(chosen, low[k], (1, 0))
        return carry

    lax.fori_loop(0, rows // 256, expand, 0)

    def activate(step, carry):
        r = pl.ds(pl.multiple_of(step * 64, 64), 64)
        g = gate[r, :]
        hidden[r, :] = (g * jax.nn.sigmoid(g) * upper[r, :]).astype(BF16)
        return carry

    lax.fori_loop(0, rows // 64, activate, 0)
    copies[2].wait()
    copies[3].start()

    def scale(step, carry):
        r = pl.ds(pl.multiple_of(step * 32, 32), 32)
        by = factor[r, :]
        for k in range(0, width, LANES):
            scaled[r, k : k + LANES] = (by * cot[r, k : k + LANES].astype(F32)).astype(BF16)
        return carry

    lax.fori_loop(0, rows // 32, scale, 0)
    blocks = hidden_units // (BLOCK * CORES)

    def outer(step, carry):
        r = pl.ds(pl.multiple_of(step * hidden_units, hidden_units), hidden_units)
        values = (mul(scaled[:, r], hidden[...], (0, 0)) * scale_out).astype(BF16)
        grad[pl.ds(step * blocks, blocks)] = values.reshape(blocks, CORES, BLOCK, hidden_units)
        return carry

    lax.fori_loop(0, width // hidden_units, outer, 0)
    halve(pos, grad, own, other)
    copies[3].wait()


def halve(pos, grad, own, other):
    count = grad.shape[0] // 16

    def step(k, carry):
        at = pl.ds(k * count, count)
        own[at] = grad[at, pos[3]]
        other[at] = grad[at, 1 - pos[3]]
        return carry

    lax.fori_loop(0, 16, step, 0)


def backward(index, gate, upper, scaled, wd, gate_sum, up_sum, d_gate, d_up):
    spots = lax.broadcasted_iota(jnp.int32, (gate_sum.shape[0], index.shape[1]), 0)
    chosen = jnp.where(index[...] == spots, 1.0, 0.0).astype(BF16)
    scale_out = wd.shape[1] ** (-0.5)

    def step(k, carry):
        r = pl.ds(pl.multiple_of(k * 256, 256), 256)
        back = mul(scaled[r, :], wd[...], (1, 0)) * scale_out
        g = gate[r, :]
        sigma = jax.nn.sigmoid(g)
        d_gate[r, :] = (back * upper[r, :] * sigma * (1.0 + g * (1.0 - sigma))).astype(BF16)
        d_up[r, :] = (back * (g * sigma)).astype(BF16)
        return carry

    lax.fori_loop(0, gate.shape[0] // 256, step, 0)
    gate_sum[...] = mul(chosen, d_gate[...], (1, 0)).astype(BF16)
    up_sum[...] = mul(chosen, d_up[...], (1, 0)).astype(BF16)


def pool_grads(pos, pool, gate_sum, up_sum, gate_own, gate_other, up_own, up_other, grad):
    width, hidden_units = pool.shape[1], gate_sum.shape[1]
    scale_in = width ** (-0.5)
    blocks = hidden_units // (BLOCK * CORES)
    for total, own, other in ((gate_sum, gate_own, gate_other), (up_sum, up_own, up_other)):

        def outer(step, carry, total=total):
            r = pl.ds(pl.multiple_of(step * hidden_units, hidden_units), hidden_units)
            values = (mul(pool[:, r], total[...], (0, 0)) * scale_in).astype(BF16)
            grad[pl.ds(step * blocks, blocks)] = values.reshape(blocks, CORES, BLOCK, hidden_units)
            return carry

        lax.fori_loop(0, width // hidden_units, outer, 0)
        halve(pos, grad, own, other)


def run_forward(pos, index, route, pool, weights, cot):
    rows, width = cot.shape
    tokens, hid = pool.shape[0], weights.shape[3]
    half = (width // (BLOCK * CORES), BLOCK, hid)
    return call(
        forward,
        [shaped(half)] * 2
        + [shaped((rows, hid), F32)] * 2
        + [shaped((rows, width)), shaped((width, hid))],
        [SMEM, VMEM, VMEM, VMEM, HBM, HBM],
        (pos, index, route, pool, weights, cot),
        scratch_shapes=[
            pltpu.VMEM((width, hid), BF16),
            pltpu.VMEM((width, hid), BF16),
            pltpu.VMEM(cot.shape, BF16),
            pltpu.VMEM((rows, LANES), F32),
            pltpu.VMEM((rows, LANES), F32),
            pltpu.VMEM((2, tokens, hid), BF16),
            pltpu.VMEM((2, tokens, hid), BF16),
            pltpu.VMEM((rows, hid), BF16),
            pltpu.VMEM((half[0], CORES, BLOCK, hid), BF16),
            pltpu.SemaphoreType.DMA((4,)),
        ],
        limit=40 * 2**20,
        work=5 * 10**9,
    )


def run_backward(index, gate, upper, scaled, wd, tokens):
    rows, hid = gate.shape
    return call(
        backward,
        [shaped((tokens, hid))] * 2,
        [VMEM] * 5,
        (index, gate, upper, scaled, wd),
        scratch_shapes=[pltpu.VMEM((rows, hid), BF16), pltpu.VMEM((rows, hid), BF16)],
        limit=24 * 2**20,
        work=3 * 10**9,
    )


def run_pool_grads(pos, pool, gate_sum, up_sum):
    width, hid = pool.shape[1], gate_sum.shape[1]
    half = (width // (BLOCK * CORES), BLOCK, hid)
    return call(
        pool_grads,
        [shaped(half)] * 4,
        [SMEM, VMEM, VMEM, VMEM],
        (pos, pool, gate_sum, up_sum),
        scratch_shapes=[pltpu.VMEM((half[0], CORES, BLOCK, hid), BF16)],
        limit=20 * 2**20,
        work=2 * 10**9,
    )


def local(
    pool_tokens,
    cotangent,
    slot_weights,
    row_index,
    route_weight,
    slot_expert,
    next_expert,
    master,
    moment_m,
    moment_v,
):
    chip = lax.axis_index("wide")
    pos = jnp.stack(
        [(chip // s) % RING for s in STRIDES] + [lax.axis_index("narrow")]
    ).astype(jnp.int32)
    slot_expert, next_expert = slot_expert[:, 0], next_expert[:, 0]
    weights_in = slot_weights
    scale_in = pool_tokens.shape[1] ** (-0.5)
    tokens = pool_tokens.shape[0]
    own, other, gate, upper, scaled, wd = run_forward(
        pos, row_index, route_weight, pool_tokens, weights_in, cotangent
    )
    cut = {2: start_grads(own, other, ORDERS[2], pos)}
    gate_sum, up_sum = run_backward(row_index, gate, upper, scaled, wd, tokens)
    cut[2], (gate_sum, up_sum) = lax.optimization_barrier((cut[2], (gate_sum, up_sum)))
    own_0, other_0, own_1, other_1 = run_pool_grads(pos, pool_tokens, gate_sum, up_sum)
    cut[0] = start_grads(own_0, other_0, ORDERS[0], pos)
    cut[1] = start_grads(own_1, other_1, ORDERS[1], pos)
    token_grads = (
        mul(gate_sum, weights_in[0, 0], (1, 1)) + mul(up_sum, weights_in[0, 1], (1, 1))
    ) * scale_in
    token_grads = token_grads.astype(BF16)

    results = {}
    out = None
    for part in (2, 0, 1):
        grads = send_grads(cut[part], ORDERS[part], pos, slot_expert)
        results[part] = update(grads, part, master, moment_m, moment_v)
        pieces = send_weights(results[part][3], ORDERS[part], pos, next_expert)
        out = assemble(pieces, ORDERS[part], part, pos, out)
    fresh, first, second = (
        jnp.stack([results[part][k] for part in range(3)], axis=1) for k in range(3)
    )
    next_weights = out.reshape(slot_weights.shape)
    return (token_grads, fresh, first, second, next_weights)


def solution(mesh):
    rows = P(("wide", "narrow"), None)
    cube = P(None, None, ("wide", "narrow"), None)
    slots = P(("wide", "narrow"), None, None, None)
    in_specs = (rows, rows, slots, rows, rows, P(), P(), cube, cube, cube)
    out_specs = (rows, cube, cube, cube, slots)
    return jax.shard_map(local, mesh=mesh, in_specs=in_specs, out_specs=out_specs, check_vma=False)
```

```python
import functools

import jax
import jax.numpy as jnp
from jax import lax
from jax.experimental import pallas as pl
from jax.experimental.pallas import tpu as pltpu
from jax.sharding import PartitionSpec as P

EXPERTS = 8
RING = 4
CORES = 2
STRIDES = (16, 4, 1)
BLOCK = 16
HIDDEN = 512
LANES = 128
VMEM_BYTES = 9 * 2**20
ORDERS = ((0, 1, 2), (1, 2, 0), (2, 0, 1))
BF16 = jnp.bfloat16
F32 = jnp.float32


VMEM = pl.BlockSpec(memory_space=pltpu.VMEM)
SMEM = pl.BlockSpec(memory_space=pltpu.SMEM)
ANY = pl.BlockSpec(memory_space=pl.ANY)
HBM = pl.BlockSpec(memory_space=pltpu.HBM)


def moved(chip, axis, steps):
    stride = STRIDES[axis]
    here = (chip // stride) % RING
    return chip + ((here + steps) % RING - here) * stride


def shift(array, axis, steps, swap=0):
    chips = RING**3
    if swap:
        pairs = [
            (CORES * chip + core, CORES * moved(chip, axis, steps) + (core ^ 1))
            for chip in range(chips)
            for core in range(CORES)
        ]
        return lax.ppermute(array, ("wide", "narrow"), pairs)
    return lax.ppermute(array, "wide", [(chip, moved(chip, axis, steps)) for chip in range(chips)])


def at_axis(ranks, axis, index, *more):
    where = [slice(None)] * ranks
    where[axis] = index
    return tuple(where) + more


def rest(order):
    return sorted(order[1:])


def slot_of(pos, order, back_a, back_b, swap):
    spot = [pos[0], pos[1], pos[2]]
    spot[order[0]] = (spot[order[0]] - back_a) & (RING - 1)
    spot[order[1]] = (spot[order[1]] - back_b) & (RING - 1)
    chip = sum(s * stride for s, stride in zip(spot, STRIDES))
    return chip * CORES + (pos[3] ^ swap)


def cut_first(order, pos, own, other, *outs):
    a = order[0]

    def step(i, carry):
        for steps in range(RING):
            target = (pos[a] + steps) & (RING - 1)
            for k, half in enumerate((own, other)):
                where = (target, i) if a == 0 else (i, *at_axis(2, a - 1, target))
                outs[steps][k, i] = half[where]
        return carry

    lax.fori_loop(0, RING, step, 0)


def cut_second(order, pos, *refs):
    ins, outs = refs[:RING], refs[RING:]
    b = order[1]
    dim = rest(order).index(b)
    for steps in range(RING):
        target = (pos[b] + steps) & (RING - 1)
        for back_a, piece in enumerate(ins):
            for k in range(CORES):
                outs[steps][CORES * back_a + k] = piece[(k,) + at_axis(2, dim, target)]


def sum_slots(order, pos, expert_of, *refs):
    ins, outs, total = refs[:4], refs[4:8], refs[8]
    d = order[2]
    total[...] = jnp.zeros_like(total)
    for back_b in range(RING):
        for k in range(RING * CORES):
            expert = expert_of[slot_of(pos, order, k // CORES, back_b, k % CORES)]
            for block in range(RING):
                total[block, expert] += ins[back_b][k, block].astype(F32)
    for steps in range(RING):
        target = (pos[d] + steps) & (RING - 1)
        outs[steps][...] = total[target].astype(outs[steps].dtype)


def adam(own, one, two, three, master, moment_m, moment_v, fresh, first, second, weights):
    grad = own[...] + one[...].astype(F32) + two[...].astype(F32) + three[...].astype(F32)
    m_next = 0.9 * moment_m[...] + 0.1 * grad
    v_next = 0.95 * moment_v[...] + 0.05 * grad * grad
    old = master[...]
    new = old - 0.05 * (m_next / (jnp.sqrt(v_next) + 1e-08) + 0.1 * old)
    fresh[...] = new
    first[...] = m_next
    second[...] = v_next
    weights[...] = new.astype(BF16)


def pick(order, pos, expert_of, *refs):
    ins, outs, sent = refs[:RING], refs[RING:-1], refs[-1]
    b, d = order[1], order[2]
    b_first = rest(order)[0] == b
    for steps in range(RING):
        for swap in range(CORES):
            expert = expert_of[slot_of(pos, order, -steps, 0, swap)]
            for back_b in range(RING):
                for back_d in range(RING):
                    at_b = (pos[b] - back_b) & (RING - 1)
                    at_d = (pos[d] - back_d) & (RING - 1)
                    spot = (at_b, at_d) if b_first else (at_d, at_b)
                    tile = ins[back_b][back_d, expert]
                    if swap:
                        sent[(steps,) + spot] = tile
                    else:
                        outs[steps][spot] = tile


def join(*refs):
    kept, other, outs = refs[:RING], refs[RING], refs[RING + 1 :]
    for steps in range(RING):
        outs[steps][0] = kept[steps][...]
        outs[steps][1] = other[steps]


def lay_out(order, pos, *refs):
    ins, out = refs[:RING], refs[-1]
    a = order[0]
    for back in range(RING):
        source = (pos[a] - back) & (RING - 1)
        for k in range(CORES):
            out[(0,) + at_axis(3, a, source, pos[3] ^ k)] = ins[back][k]


def shaped(shape, dtype=BF16):
    return jax.ShapeDtypeStruct(shape, dtype)


def call(body, outs, in_specs, args, limit=VMEM_BYTES, work=0, **more):
    specs = more.pop("out_specs", [VMEM] * len(outs))
    return pl.pallas_call(
        body,
        out_shape=outs,
        in_specs=in_specs,
        out_specs=specs,
        compiler_params=pltpu.CompilerParams(vmem_limit_bytes=limit),
        cost_estimate=pl.CostEstimate(flops=work, bytes_accessed=0, transcendentals=0),
        **more,
    )(*args)


def around(parts, axis):
    got = [parts[0]]
    for k in (2, 1, 3):
        got.append(shift(parts[k], axis, k))
    return got


def start_grads(own, other, order, pos):
    pair = (CORES, RING, RING, BLOCK, HIDDEN)
    cube = (RING, RING, RING, BLOCK, HIDDEN)
    other = lax.ppermute(other, "narrow", [(0, 1), (1, 0)])
    return call(
        functools.partial(cut_first, order),
        [shaped(pair)] * RING,
        [SMEM, VMEM, VMEM],
        (pos, own.reshape(cube), other.reshape(cube)),
    )


def send_grads(parts, order, pos, slot_expert):
    a, b, d = order
    row = (RING * CORES, RING, BLOCK, HIDDEN)
    tile = (EXPERTS, BLOCK, HIDDEN)
    parts = around(parts, a)
    parts = call(
        functools.partial(cut_second, order),
        [shaped(row)] * RING,
        [SMEM] + [VMEM] * RING,
        (pos, parts[0], parts[2], parts[1], parts[3]),
    )
    parts = around(parts, b)
    parts = call(
        functools.partial(sum_slots, order),
        [shaped(tile, F32)] + [shaped(tile)] * 3,
        [SMEM, SMEM] + [VMEM] * RING,
        (pos, slot_expert, parts[0], parts[2], parts[1], parts[3]),
        scratch_shapes=[pltpu.VMEM((RING, *tile), F32)],
    )
    parts = around(parts, d)
    return parts[0], parts[2], parts[1], parts[3]


def update(grads, part, master, moment_m, moment_v):
    tile = (EXPERTS, BLOCK, HIDDEN)
    whole = pl.BlockSpec(tile, lambda i: (0, 0, 0))
    third = pl.BlockSpec((EXPERTS, None, BLOCK, HIDDEN), lambda i: (0, part, 0, 0))
    return call(
        adam,
        [shaped(tile, F32)] * 3 + [shaped(tile)],
        [whole] * 4 + [third] * 3,
        (*grads, master, moment_m, moment_v),
        out_specs=[whole] * 4,
        grid=(1,),
    )


def send_weights(weights, order, pos, next_expert):
    a, b, d = order
    side = (RING, RING, BLOCK, HIDDEN)
    line = around([weights] * RING, d)
    line = jnp.stack([line[0], line[2], line[1], line[3]])
    plane = around([line] * RING, b)
    *kept, sent = call(
        functools.partial(pick, order),
        [shaped(side)] * RING + [shaped((RING, *side))],
        [SMEM, SMEM] + [VMEM] * RING,
        (pos, next_expert, plane[0], plane[2], plane[1], plane[3]),
    )
    other = lax.ppermute(sent, "narrow", [(0, 1), (1, 0)])
    parts = call(
        join, [shaped((CORES, *side))] * RING, [VMEM] * (RING + 1), (*kept, other)
    )
    parts = around(parts, a)
    return parts[0], parts[2], parts[1], parts[3]


def assemble(pieces, order, part, pos, into):
    dims = (3, RING, RING, RING, CORES, BLOCK, HIDDEN)
    specs = [SMEM] + [VMEM] * RING
    args = (pos, *pieces)
    alias = {}
    if into is not None:
        specs, args, alias = specs + [ANY], args + (into,), {RING + 1: 0}
    return call(
        functools.partial(lay_out, order),
        [shaped(dims)],
        specs,
        args,
        out_specs=[pl.BlockSpec((1, *dims[1:]), lambda i: (part,) + (0,) * 6)],
        grid=(1,),
        input_output_aliases=alias,
    )[0]


def mul(left, right, dims):
    return lax.dot_general(left, right, ((dims[:1], dims[1:]), ((), ())), preferred_element_type=F32)


def down_columns(row):
    return jnp.transpose(jnp.broadcast_to(row, (LANES, row.shape[1])))


def forward(pos, index, route, pool, weights_in, cot_in, own, other, gate, upper, scaled, wd,
            wg, wu, cot, spot, factor, high, low, hidden, grad, sems):
    pairs = (
        (weights_in.at[0, 0], wg),
        (weights_in.at[0, 1], wu),
        (cot_in, cot),
        (weights_in.at[0, 2], wd),
    )
    copies = [pltpu.make_async_copy(a, b, sems.at[k]) for k, (a, b) in enumerate(pairs)]
    copies[0].start()
    width, hidden_units = wg.shape
    rows = index.shape[1]
    scale_in, scale_out = width ** (-0.5), hidden_units ** (-0.5)
    spot[...] = down_columns(index[...].astype(F32))
    factor[...] = down_columns(route[...])
    for k, w in enumerate((wg, wu)):
        copies[k].wait()
        copies[k + 1].start()
        values = mul(pool[...], w[...], (1, 0)) * scale_in
        top = values.astype(BF16)
        high[k] = top
        low[k] = (values - top.astype(F32)).astype(BF16)
    lanes = lax.broadcasted_iota(jnp.int32, (256, LANES), 1).astype(F32)

    def expand(step, carry):
        r = pl.ds(pl.multiple_of(step * 256, 256), 256)
        chosen = jnp.concatenate(
            [
                jnp.where(spot[r, :] == lanes + float(k), 1.0, 0.0).astype(BF16)
                for k in range(0, pool.shape[0], LANES)
            ],
            axis=1,
        )
        for k, out in enumerate((gate, upper)):
            out[r, :] = mul(chosen, high[k], (1, 0)) + mul(chosen, low[k], (1, 0))
        return carry

    lax.fori_loop(0, rows // 256, expand, 0)

    def activate(step, carry):
        r = pl.ds(pl.multiple_of(step * 64, 64), 64)
        g = gate[r, :]
        hidden[r, :] = (g * jax.nn.sigmoid(g) * upper[r, :]).astype(BF16)
        return carry

    lax.fori_loop(0, rows // 64, activate, 0)
    copies[2].wait()
    copies[3].start()

    def scale(step, carry):
        r = pl.ds(pl.multiple_of(step * 32, 32), 32)
        by = factor[r, :]
        for k in range(0, width, LANES):
            scaled[r, k : k + LANES] = (by * cot[r, k : k + LANES].astype(F32)).astype(BF16)
        return carry

    lax.fori_loop(0, rows // 32, scale, 0)
    blocks = hidden_units // (BLOCK * CORES)

    def outer(step, carry):
        r = pl.ds(pl.multiple_of(step * hidden_units, hidden_units), hidden_units)
        values = (mul(scaled[:, r], hidden[...], (0, 0)) * scale_out).astype(BF16)
        grad[pl.ds(step * blocks, blocks)] = values.reshape(blocks, CORES, BLOCK, hidden_units)
        return carry

    lax.fori_loop(0, width // hidden_units, outer, 0)
    halve(pos, grad, own, other)
    copies[3].wait()


def halve(pos, grad, own, other):
    count = grad.shape[0] // 16

    def step(k, carry):
        at = pl.ds(k * count, count)
        own[at] = grad[at, pos[3]]
        other[at] = grad[at, 1 - pos[3]]
        return carry

    lax.fori_loop(0, 16, step, 0)


def backward(index, gate, upper, scaled, wd, gate_sum, up_sum, d_gate, d_up):
    spots = lax.broadcasted_iota(jnp.int32, (gate_sum.shape[0], index.shape[1]), 0)
    chosen = jnp.where(index[...] == spots, 1.0, 0.0).astype(BF16)
    scale_out = wd.shape[1] ** (-0.5)

    def step(k, carry):
        r = pl.ds(pl.multiple_of(k * 256, 256), 256)
        back = mul(scaled[r, :], wd[...], (1, 0)) * scale_out
        g = gate[r, :]
        sigma = jax.nn.sigmoid(g)
        d_gate[r, :] = (back * upper[r, :] * sigma * (1.0 + g * (1.0 - sigma))).astype(BF16)
        d_up[r, :] = (back * (g * sigma)).astype(BF16)
        return carry

    lax.fori_loop(0, gate.shape[0] // 256, step, 0)
    gate_sum[...] = mul(chosen, d_gate[...], (1, 0)).astype(BF16)
    up_sum[...] = mul(chosen, d_up[...], (1, 0)).astype(BF16)


def pool_grad(pos, pool, total, own, other, grad):
    width, hidden_units = pool.shape[1], total.shape[1]
    scale_in = width ** (-0.5)
    blocks = hidden_units // (BLOCK * CORES)

    def outer(step, carry):
        r = pl.ds(pl.multiple_of(step * hidden_units, hidden_units), hidden_units)
        values = (mul(pool[:, r], total[...], (0, 0)) * scale_in).astype(BF16)
        grad[pl.ds(step * blocks, blocks)] = values.reshape(blocks, CORES, BLOCK, hidden_units)
        return carry

    lax.fori_loop(0, width // hidden_units, outer, 0)
    halve(pos, grad, own, other)


def run_forward(pos, index, route, pool, weights, cot):
    rows, width = cot.shape
    tokens, hid = pool.shape[0], weights.shape[3]
    half = (width // (BLOCK * CORES), BLOCK, hid)
    return call(
        forward,
        [shaped(half)] * 2
        + [shaped((rows, hid), F32)] * 2
        + [shaped((rows, width)), shaped((width, hid))],
        [SMEM, VMEM, VMEM, VMEM, HBM, HBM],
        (pos, index, route, pool, weights, cot),
        scratch_shapes=[
            pltpu.VMEM((width, hid), BF16),
            pltpu.VMEM((width, hid), BF16),
            pltpu.VMEM(cot.shape, BF16),
            pltpu.VMEM((rows, LANES), F32),
            pltpu.VMEM((rows, LANES), F32),
            pltpu.VMEM((2, tokens, hid), BF16),
            pltpu.VMEM((2, tokens, hid), BF16),
            pltpu.VMEM((rows, hid), BF16),
            pltpu.VMEM((half[0], CORES, BLOCK, hid), BF16),
            pltpu.SemaphoreType.DMA((4,)),
        ],
        limit=40 * 2**20,
        work=5 * 10**9,
    )


def run_backward(index, gate, upper, scaled, wd, tokens):
    rows, hid = gate.shape
    return call(
        backward,
        [shaped((tokens, hid))] * 2,
        [VMEM] * 5,
        (index, gate, upper, scaled, wd),
        scratch_shapes=[pltpu.VMEM((rows, hid), BF16), pltpu.VMEM((rows, hid), BF16)],
        limit=24 * 2**20,
        work=3 * 10**9,
    )


def run_pool_grad(pos, pool, total):
    width, hid = pool.shape[1], total.shape[1]
    half = (width // (BLOCK * CORES), BLOCK, hid)
    return call(
        pool_grad,
        [shaped(half)] * 2,
        [SMEM, VMEM, VMEM],
        (pos, pool, total),
        scratch_shapes=[pltpu.VMEM((half[0], CORES, BLOCK, hid), BF16)],
        limit=16 * 2**20,
        work=10**9,
    )


def local(
    pool_tokens,
    cotangent,
    slot_weights,
    row_index,
    route_weight,
    slot_expert,
    next_expert,
    master,
    moment_m,
    moment_v,
):
    chip = lax.axis_index("wide")
    pos = jnp.stack(
        [(chip // s) % RING for s in STRIDES] + [lax.axis_index("narrow")]
    ).astype(jnp.int32)
    slot_expert, next_expert = slot_expert[:, 0], next_expert[:, 0]
    weights_in = slot_weights
    scale_in = pool_tokens.shape[1] ** (-0.5)
    tokens = pool_tokens.shape[0]
    own, other, gate, upper, scaled, wd = run_forward(
        pos, row_index, route_weight, pool_tokens, weights_in, cotangent
    )
    cut = {2: start_grads(own, other, ORDERS[2], pos)}
    gate_sum, up_sum = run_backward(row_index, gate, upper, scaled, wd, tokens)
    cut[2], (gate_sum, up_sum) = lax.optimization_barrier((cut[2], (gate_sum, up_sum)))
    for part, total in ((0, gate_sum), (1, up_sum)):
        own, other = run_pool_grad(pos, pool_tokens, total)
        cut[part] = start_grads(own, other, ORDERS[part], pos)
    token_grads = (
        mul(gate_sum, weights_in[0, 0], (1, 1)) + mul(up_sum, weights_in[0, 1], (1, 1))
    ) * scale_in
    token_grads = token_grads.astype(BF16)

    results = {}
    out = None
    for part in (2, 0, 1):
        grads = send_grads(cut[part], ORDERS[part], pos, slot_expert)
        results[part] = update(grads, part, master, moment_m, moment_v)
        pieces = send_weights(results[part][3], ORDERS[part], pos, next_expert)
        out = assemble(pieces, ORDERS[part], part, pos, out)
    fresh, first, second = (
        jnp.stack([results[part][k] for part in range(3)], axis=1) for k in range(3)
    )
    next_weights = out.reshape(slot_weights.shape)
    return (token_grads, fresh, first, second, next_weights)


def solution(mesh):
    rows = P(("wide", "narrow"), None)
    cube = P(None, None, ("wide", "narrow"), None)
    slots = P(("wide", "narrow"), None, None, None)
    in_specs = (rows, rows, slots, rows, rows, P(), P(), cube, cube, cube)
    out_specs = (rows, cube, cube, cube, slots)
    return jax.shard_map(local, mesh=mesh, in_specs=in_specs, out_specs=out_specs, check_vma=False)
```

```python
import functools

import jax
import jax.numpy as jnp
from jax import lax
from jax.experimental import pallas as pl
from jax.experimental.pallas import tpu as pltpu
from jax.sharding import PartitionSpec as P

EXPERTS = 8
RING = 4
CORES = 2
STRIDES = (16, 4, 1)
BLOCK = 16
HIDDEN = 512
LANES = 128
VMEM_BYTES = 9 * 2**20
ORDERS = ((0, 1, 2), (1, 2, 0), (2, 0, 1))
BF16 = jnp.bfloat16
F32 = jnp.float32


VMEM = pl.BlockSpec(memory_space=pltpu.VMEM)
SMEM = pl.BlockSpec(memory_space=pltpu.SMEM)
ANY = pl.BlockSpec(memory_space=pl.ANY)
HBM = pl.BlockSpec(memory_space=pltpu.HBM)


def moved(chip, axis, steps):
    stride = STRIDES[axis]
    here = (chip // stride) % RING
    return chip + ((here + steps) % RING - here) * stride


def shift(array, axis, steps, swap=0):
    chips = RING**3
    if swap:
        pairs = [
            (CORES * chip + core, CORES * moved(chip, axis, steps) + (core ^ 1))
            for chip in range(chips)
            for core in range(CORES)
        ]
        return lax.ppermute(array, ("wide", "narrow"), pairs)
    return lax.ppermute(array, "wide", [(chip, moved(chip, axis, steps)) for chip in range(chips)])


def at_axis(ranks, axis, index, *more):
    where = [slice(None)] * ranks
    where[axis] = index
    return tuple(where) + more


def rest(order):
    return sorted(order[1:])


def slot_of(pos, order, back_a, back_b, swap):
    spot = [pos[0], pos[1], pos[2]]
    spot[order[0]] = (spot[order[0]] - back_a) & (RING - 1)
    spot[order[1]] = (spot[order[1]] - back_b) & (RING - 1)
    chip = sum(s * stride for s, stride in zip(spot, STRIDES))
    return chip * CORES + (pos[3] ^ swap)


def cut_first(order, pos, own, other, *outs):
    a = order[0]

    def step(i, carry):
        for steps in range(RING):
            target = (pos[a] + steps) & (RING - 1)
            for k, half in enumerate((own, other)):
                where = (target, i) if a == 0 else (i, *at_axis(2, a - 1, target))
                outs[steps][k, i] = half[where]
        return carry

    lax.fori_loop(0, RING, step, 0)


def cut_second(order, pos, *refs):
    ins, outs = refs[:RING], refs[RING:]
    b = order[1]
    dim = rest(order).index(b)
    for steps in range(RING):
        target = (pos[b] + steps) & (RING - 1)
        for back_a, piece in enumerate(ins):
            for k in range(CORES):
                outs[steps][CORES * back_a + k] = piece[(k,) + at_axis(2, dim, target)]


def sum_slots(order, pos, expert_of, *refs):
    ins, outs, total = refs[:4], refs[4:8], refs[8]
    d = order[2]
    total[...] = jnp.zeros_like(total)
    for back_b in range(RING):
        for k in range(RING * CORES):
            expert = expert_of[slot_of(pos, order, k // CORES, back_b, k % CORES)]
            for block in range(RING):
                total[block, expert] += ins[back_b][k, block].astype(F32)
    for steps in range(RING):
        target = (pos[d] + steps) & (RING - 1)
        outs[steps][...] = total[target].astype(outs[steps].dtype)


def adam(own, one, two, three, master, moment_m, moment_v, fresh, first, second, weights):
    grad = own[...] + one[...].astype(F32) + two[...].astype(F32) + three[...].astype(F32)
    m_next = 0.9 * moment_m[...] + 0.1 * grad
    v_next = 0.95 * moment_v[...] + 0.05 * grad * grad
    old = master[...]
    new = old - 0.05 * (m_next / (jnp.sqrt(v_next) + 1e-08) + 0.1 * old)
    fresh[...] = new
    first[...] = m_next
    second[...] = v_next
    weights[...] = new.astype(BF16)


def pick(order, pos, expert_of, *refs):
    ins, outs, sent = refs[:RING], refs[RING:-1], refs[-1]
    b, d = order[1], order[2]
    b_first = rest(order)[0] == b
    for steps in range(RING):
        for swap in range(CORES):
            expert = expert_of[slot_of(pos, order, -steps, 0, swap)]
            for back_b in range(RING):
                for back_d in range(RING):
                    at_b = (pos[b] - back_b) & (RING - 1)
                    at_d = (pos[d] - back_d) & (RING - 1)
                    spot = (at_b, at_d) if b_first else (at_d, at_b)
                    tile = ins[back_b][back_d, expert]
                    if swap:
                        sent[(steps,) + spot] = tile
                    else:
                        outs[steps][spot] = tile


def join(*refs):
    kept, other, outs = refs[:RING], refs[RING], refs[RING + 1 :]
    for steps in range(RING):
        outs[steps][0] = kept[steps][...]
        outs[steps][1] = other[steps]


def lay_out(order, pos, *refs):
    ins, out = refs[:RING], refs[-1]
    a = order[0]
    y = pl.program_id(0)
    for back in range(RING):
        source = (pos[a] - back) & (RING - 1)
        for k in range(CORES):
            if a == 0:

                @pl.when(source == y)
                def _(piece=ins[back].at[k], k=k):
                    out[0, 0, :, :, pos[3] ^ k] = piece[...]

            else:
                out[(0, 0) + at_axis(2, a - 1, source, pos[3] ^ k)] = ins[back][k, y]


def shaped(shape, dtype=BF16):
    return jax.ShapeDtypeStruct(shape, dtype)


def call(body, outs, in_specs, args, limit=VMEM_BYTES, work=0, **more):
    specs = more.pop("out_specs", [VMEM] * len(outs))
    return pl.pallas_call(
        body,
        out_shape=outs,
        in_specs=in_specs,
        out_specs=specs,
        compiler_params=pltpu.CompilerParams(vmem_limit_bytes=limit),
        cost_estimate=pl.CostEstimate(flops=work, bytes_accessed=0, transcendentals=0),
        **more,
    )(*args)


def around(parts, axis):
    got = [parts[0]]
    for k in (2, 1, 3):
        got.append(shift(parts[k], axis, k))
    return got


def start_grads(own, other, order, pos):
    pair = (CORES, RING, RING, BLOCK, HIDDEN)
    cube = (RING, RING, RING, BLOCK, HIDDEN)
    other = lax.ppermute(other, "narrow", [(0, 1), (1, 0)])
    return call(
        functools.partial(cut_first, order),
        [shaped(pair)] * RING,
        [SMEM, VMEM, VMEM],
        (pos, own.reshape(cube), other.reshape(cube)),
    )


def send_grads(parts, order, pos, slot_expert):
    a, b, d = order
    row = (RING * CORES, RING, BLOCK, HIDDEN)
    tile = (EXPERTS, BLOCK, HIDDEN)
    parts = around(parts, a)
    parts = call(
        functools.partial(cut_second, order),
        [shaped(row)] * RING,
        [SMEM] + [VMEM] * RING,
        (pos, parts[0], parts[2], parts[1], parts[3]),
    )
    parts = around(parts, b)
    parts = call(
        functools.partial(sum_slots, order),
        [shaped(tile, F32)] + [shaped(tile)] * 3,
        [SMEM, SMEM] + [VMEM] * RING,
        (pos, slot_expert, parts[0], parts[2], parts[1], parts[3]),
        scratch_shapes=[pltpu.VMEM((RING, *tile), F32)],
    )
    parts = around(parts, d)
    return parts[0], parts[2], parts[1], parts[3]


def update(grads, part, master, moment_m, moment_v):
    tile = (EXPERTS, BLOCK, HIDDEN)
    whole = pl.BlockSpec(tile, lambda i: (0, 0, 0))
    third = pl.BlockSpec((EXPERTS, None, BLOCK, HIDDEN), lambda i: (0, part, 0, 0))
    return call(
        adam,
        [shaped(tile, F32)] * 3 + [shaped(tile)],
        [whole] * 4 + [third] * 3,
        (*grads, master, moment_m, moment_v),
        out_specs=[whole] * 4,
        grid=(1,),
    )


def send_weights(weights, order, pos, next_expert):
    a, b, d = order
    side = (RING, RING, BLOCK, HIDDEN)
    line = around([weights] * RING, d)
    line = jnp.stack([line[0], line[2], line[1], line[3]])
    plane = around([line] * RING, b)
    *kept, sent = call(
        functools.partial(pick, order),
        [shaped(side)] * RING + [shaped((RING, *side))],
        [SMEM, SMEM] + [VMEM] * RING,
        (pos, next_expert, plane[0], plane[2], plane[1], plane[3]),
    )
    other = lax.ppermute(sent, "narrow", [(0, 1), (1, 0)])
    parts = call(
        join, [shaped((CORES, *side))] * RING, [VMEM] * (RING + 1), (*kept, other)
    )
    parts = around(parts, a)
    return parts[0], parts[2], parts[1], parts[3]


def assemble(pieces, order, part, pos, into):
    dims = (3, RING, RING, RING, CORES, BLOCK, HIDDEN)
    specs = [SMEM] + [VMEM] * RING
    args = (pos, *pieces)
    alias = {}
    if into is not None:
        specs, args, alias = specs + [ANY], args + (into,), {RING + 1: 0}
    return call(
        functools.partial(lay_out, order),
        [shaped(dims)],
        specs,
        args,
        out_specs=[pl.BlockSpec((1, 1, *dims[2:]), lambda i: (part, i) + (0,) * 5)],
        grid=(RING,),
        input_output_aliases=alias,
    )[0]


def mul(left, right, dims):
    return lax.dot_general(left, right, ((dims[:1], dims[1:]), ((), ())), preferred_element_type=F32)


def down_columns(row):
    return jnp.transpose(jnp.broadcast_to(row, (LANES, row.shape[1])))


def forward(pos, columns, pool, weights_in, cot_in, own, other, gate, upper, scaled, wd,
            wg, wu, cot, spot, factor, high, low, hidden, grad, sems):
    pairs = (
        (weights_in.at[0, 0], wg),
        (weights_in.at[0, 1], wu),
        (cot_in, cot),
        (weights_in.at[0, 2], wd),
    )
    copies = [pltpu.make_async_copy(a, b, sems.at[k]) for k, (a, b) in enumerate(pairs)]
    copies[0].start()
    copies[1].start()
    width, hidden_units = wg.shape
    rows = columns.shape[1]
    scale_in, scale_out = width ** (-0.5), hidden_units ** (-0.5)
    spot[...] = down_columns(columns[0:1, :])
    factor[...] = down_columns(columns[1:2, :])
    for k, w in enumerate((wg, wu)):
        copies[k].wait()
        copies[k + 2].start()
        values = mul(pool[...], w[...], (1, 0)) * scale_in
        top = values.astype(BF16)
        high[k] = top
        low[k] = (values - top.astype(F32)).astype(BF16)
    lanes = lax.broadcasted_iota(jnp.int32, (256, LANES), 1).astype(F32)

    def expand(step, carry):
        r = pl.ds(pl.multiple_of(step * 256, 256), 256)
        chosen = jnp.concatenate(
            [
                jnp.where(spot[r, :] == lanes + float(k), 1.0, 0.0).astype(BF16)
                for k in range(0, pool.shape[0], LANES)
            ],
            axis=1,
        )
        for k, out in enumerate((gate, upper)):
            out[r, :] = mul(chosen, high[k], (1, 0)) + mul(chosen, low[k], (1, 0))
        return carry

    lax.fori_loop(0, rows // 256, expand, 0)

    def activate(step, carry):
        r = pl.ds(pl.multiple_of(step * 64, 64), 64)
        g = gate[r, :]
        hidden[r, :] = (g * jax.nn.sigmoid(g) * upper[r, :]).astype(BF16)
        return carry

    lax.fori_loop(0, rows // 64, activate, 0)
    copies[2].wait()

    def scale(step, carry):
        r = pl.ds(pl.multiple_of(step * 32, 32), 32)
        by = factor[r, :]
        for k in range(0, width, LANES):
            scaled[r, k : k + LANES] = (by * cot[r, k : k + LANES].astype(F32)).astype(BF16)
        return carry

    lax.fori_loop(0, rows // 32, scale, 0)
    blocks = hidden_units // (BLOCK * CORES)

    def outer(step, carry):
        r = pl.ds(pl.multiple_of(step * hidden_units, hidden_units), hidden_units)
        values = (mul(scaled[:, r], hidden[...], (0, 0)) * scale_out).astype(BF16)
        grad[pl.ds(step * blocks, blocks)] = values.reshape(blocks, CORES, BLOCK, hidden_units)
        return carry

    lax.fori_loop(0, width // hidden_units, outer, 0)
    halve(pos, grad, own, other)
    copies[3].wait()


def halve(pos, grad, own, other):
    count = grad.shape[0] // 16

    def step(k, carry):
        at = pl.ds(k * count, count)
        own[at] = grad[at, pos[3]]
        other[at] = grad[at, 1 - pos[3]]
        return carry

    lax.fori_loop(0, 16, step, 0)


def backward(columns, gate, upper, scaled, wd, gate_sum, up_sum, d_gate, d_up):
    spots = lax.broadcasted_iota(jnp.int32, (gate_sum.shape[0], columns.shape[1]), 0)
    chosen = jnp.where(columns[0:1, :] == spots.astype(F32), 1.0, 0.0).astype(BF16)
    scale_out = wd.shape[1] ** (-0.5)

    def step(k, carry):
        r = pl.ds(pl.multiple_of(k * 256, 256), 256)
        back = mul(scaled[r, :], wd[...], (1, 0)) * scale_out
        g = gate[r, :]
        sigma = jax.nn.sigmoid(g)
        d_gate[r, :] = (back * upper[r, :] * sigma * (1.0 + g * (1.0 - sigma))).astype(BF16)
        d_up[r, :] = (back * (g * sigma)).astype(BF16)
        return carry

    lax.fori_loop(0, gate.shape[0] // 256, step, 0)
    gate_sum[...] = mul(chosen, d_gate[...], (1, 0)).astype(BF16)
    up_sum[...] = mul(chosen, d_up[...], (1, 0)).astype(BF16)


def pool_grad(pos, pool, total, own, other, grad):
    width, hidden_units = pool.shape[1], total.shape[1]
    scale_in = width ** (-0.5)
    blocks = hidden_units // (BLOCK * CORES)

    def outer(step, carry):
        r = pl.ds(pl.multiple_of(step * hidden_units, hidden_units), hidden_units)
        values = (mul(pool[:, r], total[...], (0, 0)) * scale_in).astype(BF16)
        grad[pl.ds(step * blocks, blocks)] = values.reshape(blocks, CORES, BLOCK, hidden_units)
        return carry

    lax.fori_loop(0, width // hidden_units, outer, 0)
    halve(pos, grad, own, other)


def run_forward(pos, columns, pool, weights, cot):
    rows, width = cot.shape
    tokens, hid = pool.shape[0], weights.shape[3]
    half = (width // (BLOCK * CORES), BLOCK, hid)
    return call(
        forward,
        [shaped(half)] * 2
        + [shaped((rows, hid), F32)] * 2
        + [shaped((rows, width)), shaped((width, hid))],
        [SMEM, VMEM, VMEM, HBM, HBM],
        (pos, columns, pool, weights, cot),
        scratch_shapes=[
            pltpu.VMEM((width, hid), BF16),
            pltpu.VMEM((width, hid), BF16),
            pltpu.VMEM(cot.shape, BF16),
            pltpu.VMEM((rows, LANES), F32),
            pltpu.VMEM((rows, LANES), F32),
            pltpu.VMEM((2, tokens, hid), BF16),
            pltpu.VMEM((2, tokens, hid), BF16),
            pltpu.VMEM((rows, hid), BF16),
            pltpu.VMEM((half[0], CORES, BLOCK, hid), BF16),
            pltpu.SemaphoreType.DMA((4,)),
        ],
        limit=40 * 2**20,
        work=5 * 10**9,
    )


def run_backward(columns, gate, upper, scaled, wd, tokens):
    rows, hid = gate.shape
    return call(
        backward,
        [shaped((tokens, hid))] * 2,
        [VMEM] * 5,
        (columns, gate, upper, scaled, wd),
        scratch_shapes=[pltpu.VMEM((rows, hid), BF16), pltpu.VMEM((rows, hid), BF16)],
        limit=24 * 2**20,
        work=3 * 10**9,
    )


def run_pool_grad(pos, pool, total):
    width, hid = pool.shape[1], total.shape[1]
    half = (width // (BLOCK * CORES), BLOCK, hid)
    return call(
        pool_grad,
        [shaped(half)] * 2,
        [SMEM, VMEM, VMEM],
        (pos, pool, total),
        scratch_shapes=[pltpu.VMEM((half[0], CORES, BLOCK, hid), BF16)],
        limit=16 * 2**20,
        work=10**9,
    )


def local(
    pool_tokens,
    cotangent,
    slot_weights,
    row_index,
    route_weight,
    slot_expert,
    next_expert,
    master,
    moment_m,
    moment_v,
):
    chip = lax.axis_index("wide")
    pos = jnp.stack(
        [(chip // s) % RING for s in STRIDES] + [lax.axis_index("narrow")]
    ).astype(jnp.int32)
    slot_expert, next_expert = slot_expert[:, 0], next_expert[:, 0]
    weights_in = slot_weights
    scale_in = pool_tokens.shape[1] ** (-0.5)
    tokens = pool_tokens.shape[0]
    first_row = lax.broadcasted_iota(jnp.int32, (2, row_index.shape[1]), 0) == 0
    columns = jnp.where(first_row, row_index.astype(F32), route_weight)
    own, other, gate, upper, scaled, wd = run_forward(
        pos, columns, pool_tokens, weights_in, cotangent
    )
    cut = {2: start_grads(own, other, ORDERS[2], pos)}
    gate_sum, up_sum = run_backward(columns, gate, upper, scaled, wd, tokens)
    cut[2], (gate_sum, up_sum) = lax.optimization_barrier((cut[2], (gate_sum, up_sum)))
    for part, total in ((0, gate_sum), (1, up_sum)):
        own, other = run_pool_grad(pos, pool_tokens, total)
        cut[part] = start_grads(own, other, ORDERS[part], pos)
    token_grads = (
        mul(gate_sum, weights_in[0, 0], (1, 1)) + mul(up_sum, weights_in[0, 1], (1, 1))
    ) * scale_in
    token_grads = token_grads.astype(BF16)

    results = {}
    out = None
    for part in (2, 0, 1):
        grads = send_grads(cut[part], ORDERS[part], pos, slot_expert)
        results[part] = update(grads, part, master, moment_m, moment_v)
        pieces = send_weights(results[part][3], ORDERS[part], pos, next_expert)
        out = assemble(pieces, ORDERS[part], part, pos, out)
    fresh, first, second = (
        jnp.stack([results[part][k] for part in range(3)], axis=1) for k in range(3)
    )
    next_weights = out.reshape(slot_weights.shape)
    return (token_grads, fresh, first, second, next_weights)


def solution(mesh):
    rows = P(("wide", "narrow"), None)
    cube = P(None, None, ("wide", "narrow"), None)
    slots = P(("wide", "narrow"), None, None, None)
    in_specs = (rows, rows, slots, rows, rows, P(), P(), cube, cube, cube)
    out_specs = (rows, cube, cube, cube, slots)
    return jax.shard_map(local, mesh=mesh, in_specs=in_specs, out_specs=out_specs, check_vma=False)
```
